256 devices in a mesh: cfg: 64 (over z, x_lo, y), lat: 4 (over x_hi, core).
Axes of the slice: x: 4 (x_hi: 2, x_lo: 2; x = x_hi * 2 + x_lo), y: 4, z: 8, core: 2. Of those that a mesh axis runs over, the one named last changes fastest.
Arguments:
- latent_mode: float32 [128, 1048576], P('cfg', 'lat'), may hold values from -6 to 6
- latent_var: float32 [128, 1048576], P('cfg', 'lat'), may hold values from 0.05 to 2
- config_weight: float32 [128], P('cfg'), may hold values from 0.05 to 20
- grid_offset: float32 [64], replicated, may hold values from -3 to 3
Outputs:
- marginal_density: float32 [64, 1048576], P(None, ('cfg', 'lat'))
- marginal_moments: float32 [2, 1048576], P(None, ('cfg', 'lat'))
The draws below stay inside these ranges and needn't reach their ends.
All inputs are finite; a program needn't handle non-finite values.
Results may differ from the reference program's by a relative error of at most 0.00002.
Values sent between devices are 32-bit elements; how exact they have to be, the bound alone decides.
A program may use at most 64 MiB of HBM per device.

```python
import math
import jax
import jax.numpy as jnp
from jax import lax

G = 64
K = 128
NLAT = 1048576


def shard_levels(stream_key, dims, cuts, low, top_value):
    def one(dim, parts):
        steps = jax.random.uniform(jax.random.fold_in(jax.random.fold_in(stream_key, 6), dim), (parts,), jnp.float32, low / len(cuts), top_value / len(cuts))
        return jnp.repeat(jnp.exp(steps), dims[dim] // parts).reshape((-1,) + (1,) * (len(dims) - dim - 1))

    factor_of = one(*cuts[0])
    for cut in cuts[1:]:
        factor_of = factor_of * one(*cut)
    return factor_of


def scatter_about(own_key, dims, scale, limit, cuts=(), held_as=jnp.bfloat16):
    result = jax.random.normal(own_key, dims, jnp.float32) * scale
    if len(cuts) > 0:
        result = shard_levels(own_key, dims, cuts, -0.22, 0.18) * result
    return jnp.clip(result, min=-limit, max=limit).astype(held_as)


def setup_inputs(seed: int = 0) -> dict:
    key_of = jax.random.split(jax.random.key(seed), 5)
    latent_mode = scatter_about(key_of[0], (K, NLAT), 1.0, 6.0, ((0, 64), (1, 4)), jnp.float32)
    latent_var = jnp.clip(jnp.exp(math.log(2.0) - 3.6888794 * jax.random.uniform(key_of[1], (K, NLAT), jnp.float32) ** shard_levels(key_of[1], (K, NLAT), ((0, 64), (1, 4)), -0.2, 0.2)), 0.05, 2.0)
    config_weight = jnp.clip(jnp.exp(math.log(20.0) - 5.9914645 * jax.random.uniform(key_of[2], (K,), jnp.float32) ** shard_levels(key_of[2], (K,), ((0, 64),), -0.2, 0.2)), 0.05, 20.0)
    grid_offset = jnp.clip(jax.random.uniform(key_of[3], (G,), jnp.float32, -3.0, 3.0), -3.0, 3.0)
    return {"latent_mode": latent_mode, "latent_var": latent_var, "config_weight": config_weight, "grid_offset": grid_offset}


def mixture(mode_block, var_block, norm_weight, grid_offset):
    centre = lax.optimization_barrier(jnp.sum(norm_weight[:, None] * mode_block, axis=0))
    deviation = mode_block - centre[None, :]
    spread = jnp.sqrt(lax.optimization_barrier(jnp.sum(norm_weight[:, None] * (var_block + deviation * deviation), axis=0)))
    points = centre[None, :] + grid_offset[:, None] * spread[None, :]
    coefficient = norm_weight[:, None] / jnp.sqrt(6.283185307179586 * var_block)
    precision = 1.0 / var_block
    gap = points[None, :, :] - mode_block[:, None, :]
    terms = coefficient[:, None, :] * jnp.exp(-0.5 * gap * gap * precision[:, None, :])
    density = spread[None, :] * lax.optimization_barrier(jnp.sum(terms, axis=0))
    return (density, jnp.stack([centre, spread], axis=0))

def reference(latent_mode, latent_var, config_weight, grid_offset):
    norm_weight = config_weight / jnp.sum(config_weight)
    width = min(NLAT, 4096)
    count = NLAT // width
    modes_blocked = latent_mode.reshape(K, count, width).transpose(1, 0, 2)
    vars_blocked = latent_var.reshape(K, count, width).transpose(1, 0, 2)

    def one_block(pair):
        return mixture(pair[0], pair[1], norm_weight, grid_offset)
    density, moments = lax.map(one_block, (modes_blocked, vars_blocked))
    density = density.transpose(1, 0, 2).reshape(G, NLAT)
    moments = moments.transpose(1, 0, 2).reshape(2, NLAT)
    return (density, moments)
```

```python
import functools
import math

import jax
import jax.numpy as jnp
from jax import lax
from jax.experimental import pallas as pl
from jax.experimental.pallas import tpu as pltpu
from jax.sharding import PartitionSpec as P

MESH = pl.DeviceIdType.MESH
LANES = 128
CHUNKS = 4
AHEAD = 2
GROUP = 16
LOG2E = 1.4426950408889634


def pair_sum(x, even):
    return x + jnp.where(even, pltpu.roll(x, 7, 0), pltpu.roll(x, 1, 0))


def kernel(n_cfg, n_lat, mode, var, weight, offset, dens, mom, buf, wbuf, wnorm, coef, send_sem, recv_sem, wsend_sem, wrecv_sem):
    c = lax.axis_index("cfg")
    l = lax.axis_index("lat")
    dests = n_cfg
    rows = mode.shape[0] // dests
    size = rows // CHUNKS
    near = n_cfg // n_lat
    first = l * near
    turn = lax.rem(c * 4 + l, dests)

    def target(i):
        d = lax.rem(i + turn, dests)
        return d, first + d // n_lat, lax.rem(d, n_lat)

    def each(i, do_local, do_remote):
        d, tc, tl = target(i)
        own = jnp.logical_and(tc == c, tl == l)

        @pl.when(own)
        def _():
            do_local(d)

        @pl.when(jnp.logical_not(own))
        def _():
            do_remote(d, tc, tl)

    def send_weights(i, carry):
        def local(d):
            pltpu.make_async_copy(weight, wbuf.at[c], wrecv_sem).start()

        def remote(d, tc, tl):
            pltpu.make_async_remote_copy(
                src_ref=weight, dst_ref=wbuf.at[c], send_sem=wsend_sem, recv_sem=wrecv_sem,
                device_id=(tc, tl), device_id_type=MESH,
            ).start()

        each(i, local, remote)
        return carry

    def send_chunk(j):
        def body(i, carry):
            def src(ref, d):
                return ref.at[pl.ds(pl.multiple_of(d * rows + j * size, 8), size)]

            def local(d):
                for a, ref in enumerate((mode, var)):
                    pltpu.make_async_copy(src(ref, d), buf.at[j, a, c], recv_sem.at[j]).start()

            def remote(d, tc, tl):
                for a, ref in enumerate((mode, var)):
                    pltpu.make_async_remote_copy(
                        src_ref=src(ref, d), dst_ref=buf.at[j, a, c], send_sem=send_sem.at[j], recv_sem=recv_sem.at[j],
                        device_id=(tc, tl), device_id_type=MESH,
                    ).start()

            each(i, local, remote)
            return carry

        lax.fori_loop(0, dests, body, 0)

    lax.fori_loop(0, dests, send_weights, 0)
    for j in range(min(AHEAD, CHUNKS)):
        send_chunk(j)

    parity = lax.broadcasted_iota(jnp.int32, (8, LANES), 0)
    even = lax.rem(parity, 2) == 0

    pltpu.make_async_copy(wbuf, wbuf, wrecv_sem).wait()

    def spread_weight(s, total):
        w = jnp.where(even, jnp.broadcast_to(wbuf[s, 0:1, :], (8, LANES)), jnp.broadcast_to(wbuf[s, 1:2, :], (8, LANES)))
        wnorm[s] = w
        return total + w

    total = lax.fori_loop(0, n_cfg, spread_weight, jnp.zeros((8, LANES), jnp.float32), unroll=8)
    total = pair_sum(total, even)

    def divide_weight(s, carry):
        wnorm[s] = wnorm[s] / total
        return carry

    lax.fori_loop(0, n_cfg, divide_weight, 0, unroll=8)

    zero = jnp.zeros((8, LANES), jnp.float32)
    for j in range(CHUNKS):
        pltpu.make_async_copy(buf.at[j], buf.at[j], recv_sem.at[j]).wait()

        def tile(q, carry):
            at = pl.ds(pl.multiple_of(q * 8, 8), 8)

            def first_moment(s, acc):
                return acc + wnorm[s] * buf[j, 0, s, at, :]

            centre = pair_sum(lax.fori_loop(0, n_cfg, first_moment, zero, unroll=8), even)

            def second_moment(s, acc):
                dev = buf[j, 0, s, at, :] - centre
                return acc + wnorm[s] * (buf[j, 1, s, at, :] + dev * dev)

            spread = jnp.sqrt(pair_sum(lax.fori_loop(0, n_cfg, second_moment, zero, unroll=8), even))

            def prepare(s, carry):
                root = lax.rsqrt(buf[j, 1, s, at, :])
                scale = root * math.sqrt(0.5 * LOG2E)
                coef[0, s] = scale * (centre - buf[j, 0, s, at, :])
                coef[1, s] = scale * spread
                coef[2, s] = wnorm[s] * root * (1.0 / math.sqrt(2.0 * math.pi))
                return carry

            lax.fori_loop(0, n_cfg, prepare, 0, unroll=8)

            column = (j * size + q * 8) * (LANES // 2)
            for t in range(4):
                lanes = pl.ds(pl.multiple_of(column + t * LANES, LANES), LANES)
                mom[0:1, lanes] = centre[2 * t : 2 * t + 1, :]
                mom[1:2, lanes] = spread[2 * t : 2 * t + 1, :]

            for base in range(0, dens.shape[0], GROUP):
                grid = [jnp.full((8, LANES), offset[base + g], jnp.float32) for g in range(GROUP)]

                def add_source(s, accs):
                    a, b, k = coef[0, s], coef[1, s], coef[2, s]
                    out = []
                    for g in range(GROUP):
                        x = a + grid[g] * b
                        out.append(accs[g] + k * jnp.exp2(-(x * x)))
                    return tuple(out)

                accs = lax.fori_loop(0, n_cfg, add_source, (zero,) * GROUP, unroll=2)
                for g in range(GROUP):
                    value = spread * pair_sum(accs[g], even)
                    for t in range(4):
                        lanes = pl.ds(pl.multiple_of(column + t * LANES, LANES), LANES)
                        dens[base + g : base + g + 1, lanes] = value[2 * t : 2 * t + 1, :]
            return carry

        if j + AHEAD < CHUNKS:
            send_chunk(j + AHEAD)
        lax.fori_loop(0, size // 8, tile, 0)

    def finish(i, carry):
        _, tc, tl = target(i)
        own = jnp.logical_and(tc == c, tl == l)

        @pl.when(jnp.logical_not(own))
        def _():
            pltpu.make_async_copy(weight, wbuf.at[0], wsend_sem).wait()
            for j in range(CHUNKS):
                pltpu.make_async_copy(buf.at[j, :, 0], buf.at[j, :, 0], send_sem.at[j]).wait()

        return carry

    lax.fori_loop(0, dests, finish, 0)


def per_device(latent_mode, latent_var, config_weight, grid_offset):
    n_cfg = lax.axis_size("cfg")
    n_lat = lax.axis_size("lat")
    own, width = latent_mode.shape
    grid = grid_offset.shape[0]
    lat_dev = width // n_cfg

    def rows(a):
        return a.reshape(own, width // LANES, LANES).transpose(1, 0, 2).reshape(own * width // LANES, LANES)

    weight = jnp.broadcast_to(config_weight[:, None], (own, LANES))
    block = own * lat_dev // LANES
    vmem = pl.BlockSpec(memory_space=pltpu.VMEM)
    hbm = pl.BlockSpec(memory_space=pl.ANY)
    return pl.pallas_call(
        functools.partial(kernel, n_cfg, n_lat),
        out_shape=(
            jax.ShapeDtypeStruct((grid, lat_dev), jnp.float32),
            jax.ShapeDtypeStruct((2, lat_dev), jnp.float32),
        ),
        in_specs=[hbm, hbm, vmem, pl.BlockSpec(memory_space=pltpu.SMEM)],
        out_specs=(vmem, vmem),
        scratch_shapes=[
            pltpu.VMEM((CHUNKS, 2, n_cfg, block // CHUNKS, LANES), jnp.float32),
            pltpu.VMEM((n_cfg, own, LANES), jnp.float32),
            pltpu.VMEM((n_cfg, 8, LANES), jnp.float32),
            pltpu.VMEM((3, n_cfg, 8, LANES), jnp.float32),
            pltpu.SemaphoreType.DMA((CHUNKS,)),
            pltpu.SemaphoreType.DMA((CHUNKS,)),
            pltpu.SemaphoreType.DMA,
            pltpu.SemaphoreType.DMA,
        ],
        compiler_params=pltpu.CompilerParams(has_side_effects=True, vmem_limit_bytes=40 * 1024 * 1024),
        name="mixture",
    )(rows(latent_mode), rows(latent_var), weight, grid_offset)


def solution(mesh):
    return jax.shard_map(
        per_device,
        mesh=mesh,
        in_specs=(P("cfg", "lat"), P("cfg", "lat"), P("cfg"), P()),
        out_specs=(P(None, ("cfg", "lat")), P(None, ("cfg", "lat"))),
        check_vma=False,
    )
```

```python
import functools
import math

import jax
import jax.numpy as jnp
from jax import lax
from jax.experimental import pallas as pl
from jax.experimental.pallas import tpu as pltpu
from jax.sharding import PartitionSpec as P

MESH = pl.DeviceIdType.MESH
LANES = 128
CHUNKS = 8
LAG = 2
GROUP = 16
LOG2E = 1.4426950408889634
NZ, NX, NY = 8, 2, 4


def pair_sum(x, even):
    return x + jnp.where(even, pltpu.roll(x, 7, 0), pltpu.roll(x, 1, 0))


def kernel(n_lat, mode, var, weight, offset, dens, mom, relay, buf, wbuf, wnorm, coef, sem1, sem2, wsem):
    c = lax.axis_index("cfg")
    l = lax.axis_index("lat")
    z, xl, y = c // (NX * NY), (c // NY) % NX, c % NY
    row = xl * n_lat + l
    n_row = NX * n_lat
    plane = z * NY + y
    n_plane = NZ * NY
    n_cfg = NZ * NX * NY
    size = buf.shape[3]

    def remote(src, dst, send, recv, device):
        return pltpu.make_async_remote_copy(
            src_ref=src, dst_ref=dst, send_sem=send, recv_sem=recv, device_id=device, device_id_type=MESH)

    def first_hop(j):
        def ends(i):
            t = lax.rem(i + row, n_row)
            tx, tl = t // n_lat, lax.rem(t, n_lat)
            rows = pl.ds(j * size, size)
            return tx, tl, [(ref.at[:, tx, :, tl, rows], relay.at[j, l, :, :, xl, a]) for a, ref in enumerate((mode, var))]

        for src, dst in ends(0)[2]:
            pltpu.make_async_copy(src, dst, sem1.at[1, j]).start()

        def body(i, carry):
            tx, tl, pairs = ends(i)
            for src, dst in pairs:
                remote(src, dst, sem1.at[0, j], sem1.at[1, j], (z * NX * NY + tx * NY + y, tl)).start()
            return carry

        lax.fori_loop(1, n_row, body, 0)

    def second_hop(j):
        pltpu.make_async_copy(relay.at[j], relay.at[j], sem1.at[1, j]).wait()
        mine = pl.ds(plane * NX, NX)

        def body(i, carry):
            tz = lax.rem(z + 3 * i, NZ)
            ty = lax.rem(y + i // NZ, NY)
            remote(relay.at[j, tz // 2, lax.rem(tz, 2), ty], buf.at[j, mine], sem2.at[0, j], sem2.at[1, j],
                   (tz * NX * NY + xl * NY + ty, l)).start()
            return carry

        lax.fori_loop(1, n_plane, body, 0)
        buf[j, mine] = relay[j, z // 2, lax.rem(z, 2), y]

    def send_weights(i, carry):
        d = lax.rem(i + c, n_cfg)
        tc, tl = l * (n_cfg // n_lat) + d // n_lat, lax.rem(d, n_lat)
        own = jnp.logical_and(tc == c, tl == l)
        slot = wbuf.at[plane * NX + xl]

        @pl.when(own)
        def _():
            slot[...] = weight[...]

        @pl.when(jnp.logical_not(own))
        def _():
            remote(weight, slot, wsem.at[0], wsem.at[1], (tc, tl)).start()

        return carry

    for j in range(CHUNKS):
        first_hop(j)
    lax.fori_loop(0, n_cfg, send_weights, 0)

    parity = lax.broadcasted_iota(jnp.int32, (8, LANES), 0)
    even = lax.rem(parity, 2) == 0
    zero = jnp.zeros((8, LANES), jnp.float32)
    receives_own = z // 2 == l

    def normalize_weights():
        @pl.when(receives_own)
        def _():
            pltpu.make_async_copy(wbuf.at[pl.ds(0, n_cfg - 1)], wbuf.at[pl.ds(0, n_cfg - 1)], wsem.at[1]).wait()

        @pl.when(jnp.logical_not(receives_own))
        def _():
            pltpu.make_async_copy(wbuf, wbuf, wsem.at[1]).wait()

        def spread_weight(s, total):
            w = jnp.where(even, jnp.broadcast_to(wbuf[s, 0:1, :], (8, LANES)), jnp.broadcast_to(wbuf[s, 1:2, :], (8, LANES)))
            wnorm[s] = w
            return total + w

        total = pair_sum(lax.fori_loop(0, n_cfg, spread_weight, zero, unroll=8), even)

        def divide_weight(s, carry):
            wnorm[s] = wnorm[s] / total
            return carry

        lax.fori_loop(0, n_cfg, divide_weight, 0, unroll=8)

    def evaluate(j):
        pltpu.make_async_copy(buf.at[j, pl.ds(0, n_cfg - NX)], buf.at[j, pl.ds(0, n_cfg - NX)], sem2.at[1, j]).wait()

        def tile(q, carry):
            at = pl.ds(pl.multiple_of(q * 8, 8), 8)

            def first_moment(s, acc):
                return acc + wnorm[s] * buf[j, s, 0, at, :]

            centre = pair_sum(lax.fori_loop(0, n_cfg, first_moment, zero, unroll=8), even)

            def second_moment(s, acc):
                dev = buf[j, s, 0, at, :] - centre
                return acc + wnorm[s] * (buf[j, s, 1, at, :] + dev * dev)

            spread = jnp.sqrt(pair_sum(lax.fori_loop(0, n_cfg, second_moment, zero, unroll=8), even))

            def prepare(s, carry):
                root = lax.rsqrt(buf[j, s, 1, at, :])
                scale = root * math.sqrt(0.5 * LOG2E)
                coef[0, s] = scale * (centre - buf[j, s, 0, at, :])
                coef[1, s] = scale * spread
                coef[2, s] = wnorm[s] * root * (1.0 / math.sqrt(2.0 * math.pi))
                return carry

            lax.fori_loop(0, n_cfg, prepare, 0, unroll=8)

            column = (j * size + q * 8) * (LANES // 2)
            for t in range(4):
                lanes = pl.ds(pl.multiple_of(column + t * LANES, LANES), LANES)
                mom[0:1, lanes] = centre[2 * t : 2 * t + 1, :]
                mom[1:2, lanes] = spread[2 * t : 2 * t + 1, :]

            for base in range(0, dens.shape[0], GROUP):
                grid = [jnp.full((8, LANES), offset[base + g], jnp.float32) for g in range(GROUP)]

                def add_source(s, accs):
                    a, b, k = coef[0, s], coef[1, s], coef[2, s]
                    out = []
                    for g in range(GROUP):
                        x = a + grid[g] * b
                        out.append(accs[g] + k * jnp.exp2(-(x * x)))
                    return tuple(out)

                accs = lax.fori_loop(0, n_cfg, add_source, (zero,) * GROUP, unroll=2)
                for g in range(GROUP):
                    value = spread * pair_sum(accs[g], even)
                    for t in range(4):
                        lanes = pl.ds(pl.multiple_of(column + t * LANES, LANES), LANES)
                        dens[base + g : base + g + 1, lanes] = value[2 * t : 2 * t + 1, :]
            return carry

        lax.fori_loop(0, size // 8, tile, 0)

    def evaluate_step(j, carry):
        evaluate(j)
        return carry

    for j in range(CHUNKS):
        second_hop(j)
        if j == LAG - 1:
            normalize_weights()
        if j >= LAG:
            lax.fori_loop(j - LAG, j - LAG + 1, evaluate_step, 0)
    lax.fori_loop(CHUNKS - LAG, CHUNKS, evaluate_step, 0)

    def finish_first(i, carry):
        for j in range(CHUNKS):
            for a in range(2):
                pltpu.make_async_copy(relay.at[j, 0, :, :, 0, a], relay.at[j, 0, :, :, 0, a], sem1.at[0, j]).wait()
        return carry

    lax.fori_loop(1, n_row, finish_first, 0)
    for j in range(CHUNKS):
        pltpu.make_async_copy(buf.at[j, pl.ds(0, n_cfg - NX)], buf.at[j, pl.ds(0, n_cfg - NX)], sem2.at[0, j]).wait()

    @pl.when(receives_own)
    def _():
        pltpu.make_async_copy(wbuf.at[pl.ds(0, n_cfg - 1)], wbuf.at[pl.ds(0, n_cfg - 1)], wsem.at[0]).wait()

    @pl.when(jnp.logical_not(receives_own))
    def _():
        pltpu.make_async_copy(wbuf, wbuf, wsem.at[0]).wait()


def per_device(latent_mode, latent_var, config_weight, grid_offset):
    n_cfg = lax.axis_size("cfg")
    n_lat = lax.axis_size("lat")
    own, width = latent_mode.shape
    grid = grid_offset.shape[0]
    lat_dev = width // n_cfg
    block = own * lat_dev // LANES
    size = block // CHUNKS

    def rows(a):
        a = a.reshape(own, width // LANES, LANES).transpose(1, 0, 2)
        return a.reshape(n_cfg // n_lat // (NX * NY), NX, NY, n_lat, block, LANES)

    weight = jnp.broadcast_to(config_weight[:, None], (own, LANES))
    vmem = pl.BlockSpec(memory_space=pltpu.VMEM)
    hbm = pl.BlockSpec(memory_space=pl.ANY)
    return pl.pallas_call(
        functools.partial(kernel, n_lat),
        out_shape=(
            jax.ShapeDtypeStruct((grid, lat_dev), jnp.float32),
            jax.ShapeDtypeStruct((2, lat_dev), jnp.float32),
        ),
        in_specs=[hbm, hbm, vmem, pl.BlockSpec(memory_space=pltpu.SMEM)],
        out_specs=(vmem, vmem),
        scratch_shapes=[
            pltpu.VMEM((CHUNKS, n_lat, NZ // n_lat, NY, NX, 2, size, LANES), jnp.float32),
            pltpu.VMEM((CHUNKS, n_cfg, 2, size, LANES), jnp.float32),
            pltpu.VMEM((n_cfg, own, LANES), jnp.float32),
            pltpu.VMEM((n_cfg, 8, LANES), jnp.float32),
            pltpu.VMEM((3, n_cfg, 8, LANES), jnp.float32),
            pltpu.SemaphoreType.DMA((2, CHUNKS)),
            pltpu.SemaphoreType.DMA((2, CHUNKS)),
            pltpu.SemaphoreType.DMA((2,)),
        ],
        compiler_params=pltpu.CompilerParams(has_side_effects=True, vmem_limit_bytes=61 * 1024 * 1024),
        name="mixture",
    )(rows(latent_mode), rows(latent_var), weight, grid_offset)


def solution(mesh):
    return jax.shard_map(
        per_device,
        mesh=mesh,
        in_specs=(P("cfg", "lat"), P("cfg", "lat"), P("cfg"), P()),
        out_specs=(P(None, ("cfg", "lat")), P(None, ("cfg", "lat"))),
        check_vma=False,
    )
```

```python
import functools
import math

import jax
import jax.numpy as jnp
from jax import lax
from jax.experimental import pallas as pl
from jax.experimental.pallas import tpu as pltpu
from jax.sharding import PartitionSpec as P

MESH = pl.DeviceIdType.MESH
LANES = 128
CHUNKS = 8
LAG = 2
AHEAD = 1
GROUP = 16
LOG2E = 1.4426950408889634
NZ, NX, NY = 8, 2, 4


def pair_sum(x, even):
    return x + jnp.where(even, pltpu.roll(x, 7, 0), pltpu.roll(x, 1, 0))


def kernel(n_lat, mode, var, weight, offset, dens, mom, relay, buf, wpair, wbuf, wnorm, coef, sem1, sem2, wsem):
    c = lax.axis_index("cfg")
    l = lax.axis_index("lat")
    z, xl, y = c // (NX * NY), (c // NY) % NX, c % NY
    row = xl * n_lat + l
    n_row = NX * n_lat
    plane = z * NY + y
    n_plane = NZ * NY
    n_cfg = NZ * NX * NY
    size = buf.shape[3]

    def remote(src, dst, send, recv, device):
        return pltpu.make_async_remote_copy(
            src_ref=src, dst_ref=dst, send_sem=send, recv_sem=recv, device_id=device, device_id_type=MESH)

    def first_hop_own(j):
        rows = pl.ds(j * size, size)
        for a, ref in enumerate((mode, var)):
            pltpu.make_async_copy(ref.at[:, xl, :, l, rows], relay.at[j, l, :, :, xl, a], sem1.at[1, j]).start()

    def first_hop_send(j, i):
        t = lax.rem(i + row, n_row)
        tx, tl = t // n_lat, lax.rem(t, n_lat)
        rows = pl.ds(j * size, size)
        for a, ref in enumerate((mode, var)):
            remote(ref.at[:, tx, :, tl, rows], relay.at[j, l, :, :, xl, a], sem1.at[0, j], sem1.at[1, j],
                   (z * NX * NY + tx * NY + y, tl)).start()

    def plane_peer(i):
        tz = lax.rem(z + 3 * i, NZ)
        ty = lax.rem(y + i // NZ, NY)
        return tz, ty, (tz * NX * NY + xl * NY + ty, l)

    mine = pl.ds(plane * NX, NX)

    def second_hop_send(j, i):
        tz, ty, device = plane_peer(i)
        remote(relay.at[j, tz // 2, lax.rem(tz, 2), ty], buf.at[j, mine], sem2.at[0, j], sem2.at[1, j], device).start()

    def second_hop(j):
        if j + AHEAD < CHUNKS:
            first_hop_own(j + AHEAD)
        pltpu.make_async_copy(relay.at[j], relay.at[j], sem1.at[1, j]).wait()
        share = (n_plane - 1) // (n_row - 1)

        def body(i, carry):
            if j + AHEAD < CHUNKS:
                first_hop_send(j + AHEAD, i + 1)
            for k in range(share):
                second_hop_send(j, i * share + k + 1)
            return carry

        lax.fori_loop(0, n_row - 1, body, 0)
        for i in range((n_row - 1) * share + 1, n_plane):
            second_hop_send(j, i)
        buf[j, mine] = relay[j, z // 2, lax.rem(z, 2), y]

    for r in range(2):
        wpair[xl, r : r + 1, :] = jnp.full((1, LANES), weight[r], jnp.float32)

    barrier = pltpu.get_barrier_semaphore()

    def greet_row(i, carry):
        t = lax.rem(i + row, n_row)
        pl.semaphore_signal(barrier, inc=1, device_id=(z * NX * NY + (t // n_lat) * NY + y, lax.rem(t, n_lat)), device_id_type=MESH)
        return carry

    def greet_plane(i, carry):
        pl.semaphore_signal(barrier, inc=1, device_id=plane_peer(i)[2], device_id_type=MESH)
        return carry

    lax.fori_loop(1, n_plane, greet_plane, 0)
    lax.fori_loop(1, n_row, greet_row, 0)
    pl.semaphore_wait(barrier, n_plane + n_row - 2)

    pair_copy = remote(wpair.at[xl], wpair.at[xl], wsem.at[0], wsem.at[1], (z * NX * NY + (1 - xl) * NY + y, l))
    pair_copy.start()
    for j in range(min(AHEAD, CHUNKS)):
        first_hop_own(j)

        def start_row(i, carry):
            first_hop_send(j, i)
            return carry

        lax.fori_loop(1, n_row, start_row, 0)

    def send_weights():
        pair_copy.wait()

        def body(i, carry):
            remote(wpair, wbuf.at[mine], wsem.at[2], wsem.at[3], plane_peer(i)[2]).start()
            return carry

        lax.fori_loop(1, n_plane, body, 0)
        wbuf[mine] = wpair[...]

    parity = lax.broadcasted_iota(jnp.int32, (8, LANES), 0)
    even = lax.rem(parity, 2) == 0
    zero = jnp.zeros((8, LANES), jnp.float32)

    def normalize_weights():
        pltpu.make_async_copy(wbuf.at[pl.ds(0, n_cfg - NX)], wbuf.at[pl.ds(0, n_cfg - NX)], wsem.at[3]).wait()

        def spread_weight(s, total):
            w = jnp.where(even, jnp.broadcast_to(wbuf[s, 0:1, :], (8, LANES)), jnp.broadcast_to(wbuf[s, 1:2, :], (8, LANES)))
            wnorm[s] = w
            return total + w

        total = pair_sum(lax.fori_loop(0, n_cfg, spread_weight, zero, unroll=8), even)

        def divide_weight(s, carry):
            wnorm[s] = wnorm[s] / total
            return carry

        lax.fori_loop(0, n_cfg, divide_weight, 0, unroll=8)

    def evaluate(j):
        pltpu.make_async_copy(buf.at[j, pl.ds(0, n_cfg - NX)], buf.at[j, pl.ds(0, n_cfg - NX)], sem2.at[1, j]).wait()

        def tile(q, carry):
            at = pl.ds(pl.multiple_of(q * 8, 8), 8)

            def first_moment(s, acc):
                return acc + wnorm[s] * buf[j, s, 0, at, :]

            centre = pair_sum(lax.fori_loop(0, n_cfg, first_moment, zero, unroll=8), even)

            def second_moment(s, acc):
                dev = buf[j, s, 0, at, :] - centre
                return acc + wnorm[s] * (buf[j, s, 1, at, :] + dev * dev)

            spread = jnp.sqrt(pair_sum(lax.fori_loop(0, n_cfg, second_moment, zero, unroll=8), even))

            def prepare(s, carry):
                root = lax.rsqrt(buf[j, s, 1, at, :])
                scale = root * math.sqrt(0.5 * LOG2E)
                coef[0, s] = scale * (centre - buf[j, s, 0, at, :])
                coef[1, s] = scale * spread
                coef[2, s] = wnorm[s] * root * (1.0 / math.sqrt(2.0 * math.pi))
                return carry

            lax.fori_loop(0, n_cfg, prepare, 0, unroll=8)

            column = (j * size + q * 8) * (LANES // 2)
            for t in range(4):
                lanes = pl.ds(pl.multiple_of(column + t * LANES, LANES), LANES)
                mom[0:1, lanes] = centre[2 * t : 2 * t + 1, :]
                mom[1:2, lanes] = spread[2 * t : 2 * t + 1, :]

            for base in range(0, dens.shape[0], GROUP):
                grid = [jnp.full((8, LANES), offset[base + g], jnp.float32) for g in range(GROUP)]

                def add_source(s, accs):
                    a, b, k = coef[0, s], coef[1, s], coef[2, s]
                    out = []
                    for g in range(GROUP):
                        x = a + grid[g] * b
                        out.append(accs[g] + k * jnp.exp2(-(x * x)))
                    return tuple(out)

                accs = lax.fori_loop(0, n_cfg, add_source, (zero,) * GROUP, unroll=2)
                for g in range(GROUP):
                    value = spread * pair_sum(accs[g], even)
                    for t in range(4):
                        lanes = pl.ds(pl.multiple_of(column + t * LANES, LANES), LANES)
                        dens[base + g : base + g + 1, lanes] = value[2 * t : 2 * t + 1, :]
            return carry

        lax.fori_loop(0, size // 8, tile, 0)

    def evaluate_step(j, carry):
        evaluate(j)
        return carry

    for j in range(CHUNKS):
        second_hop(j)
        if j == 0:
            send_weights()
        if j == LAG - 1:
            normalize_weights()
        if j >= LAG:
            lax.fori_loop(j - LAG, j - LAG + 1, evaluate_step, 0)
    lax.fori_loop(CHUNKS - LAG, CHUNKS, evaluate_step, 0)

    def finish_first(i, carry):
        for j in range(CHUNKS):
            for a in range(2):
                pltpu.make_async_copy(relay.at[j, 0, :, :, 0, a], relay.at[j, 0, :, :, 0, a], sem1.at[0, j]).wait()
        return carry

    lax.fori_loop(1, n_row, finish_first, 0)
    for j in range(CHUNKS):
        pltpu.make_async_copy(buf.at[j, pl.ds(0, n_cfg - NX)], buf.at[j, pl.ds(0, n_cfg - NX)], sem2.at[0, j]).wait()

    pltpu.make_async_copy(wbuf.at[pl.ds(0, n_cfg - NX)], wbuf.at[pl.ds(0, n_cfg - NX)], wsem.at[2]).wait()


def per_device(latent_mode, latent_var, config_weight, grid_offset):
    n_cfg = lax.axis_size("cfg")
    n_lat = lax.axis_size("lat")
    own, width = latent_mode.shape
    grid = grid_offset.shape[0]
    lat_dev = width // n_cfg
    block = own * lat_dev // LANES
    size = block // CHUNKS

    def rows(a):
        a = a.reshape(own, width // LANES, LANES).transpose(1, 0, 2)
        return a.reshape(n_cfg // n_lat // (NX * NY), NX, NY, n_lat, block, LANES)

    vmem = pl.BlockSpec(memory_space=pltpu.VMEM)
    smem = pl.BlockSpec(memory_space=pltpu.SMEM)
    hbm = pl.BlockSpec(memory_space=pl.ANY)
    return pl.pallas_call(
        functools.partial(kernel, n_lat),
        out_shape=(
            jax.ShapeDtypeStruct((grid, lat_dev), jnp.float32),
            jax.ShapeDtypeStruct((2, lat_dev), jnp.float32),
        ),
        in_specs=[hbm, hbm, smem, smem],
        out_specs=(vmem, vmem),
        scratch_shapes=[
            pltpu.VMEM((CHUNKS, n_lat, NZ // n_lat, NY, NX, 2, size, LANES), jnp.float32),
            pltpu.VMEM((CHUNKS, n_cfg, 2, size, LANES), jnp.float32),
            pltpu.VMEM((NX, own, LANES), jnp.float32),
            pltpu.VMEM((n_cfg, own, LANES), jnp.float32),
            pltpu.VMEM((n_cfg, 8, LANES), jnp.float32),
            pltpu.VMEM((3, n_cfg, 8, LANES), jnp.float32),
            pltpu.SemaphoreType.DMA((2, CHUNKS)),
            pltpu.SemaphoreType.DMA((2, CHUNKS)),
            pltpu.SemaphoreType.DMA((4,)),
        ],
        compiler_params=pltpu.CompilerParams(collective_id=0, has_side_effects=True, vmem_limit_bytes=61 * 1024 * 1024),
        name="mixture",
    )(rows(latent_mode), rows(latent_var), config_weight, grid_offset)


def solution(mesh):
    return jax.shard_map(
        per_device,
        mesh=mesh,
        in_specs=(P("cfg", "lat"), P("cfg", "lat"), P("cfg"), P()),
        out_specs=(P(None, ("cfg", "lat")), P(None, ("cfg", "lat"))),
        check_vma=False,
    )
```

```python
import functools
import math

import jax
import jax.numpy as jnp
from jax import lax
from jax.experimental import pallas as pl
from jax.experimental.pallas import tpu as pltpu
from jax.sharding import PartitionSpec as P

MESH = pl.DeviceIdType.MESH
LANES = 128
CHUNKS = 8
LAG = 2
AHEAD = 2
GROUP = 16
LOG2E = 1.4426950408889634
NZ, NX, NY = 8, 2, 4
LAT_ORDER = (0, 2, 1, 3)
ROW_ORDER = ((1, 0), (0, 2), (1, 2), (0, 1), (1, 1), (0, 3), (1, 3))


def pair_sum(x, even):
    return x + jnp.where(even, pltpu.roll(x, 7, 0), pltpu.roll(x, 1, 0))


def kernel(n_lat, mode, var, weight, offset, dens, mom, relay, buf, wpair, wbuf, wnorm, coef, sem1, sem1r, sem2, wsem):
    c = lax.axis_index("cfg")
    l = lax.axis_index("lat")
    z, xl, y = c // (NX * NY), (c // NY) % NX, c % NY
    n_row = NX * n_lat
    plane = z * NY + y
    n_plane = NZ * NY
    n_cfg = NZ * NX * NY
    size = buf.shape[3]

    def remote(src, dst, send, recv, device):
        return pltpu.make_async_remote_copy(
            src_ref=src, dst_ref=dst, send_sem=send, recv_sem=recv, device_id=device, device_id_type=MESH)

    def first_hop_own(j):
        rows = pl.ds(j * size, size)
        for a, ref in enumerate((mode, var)):
            pltpu.make_async_copy(ref.at[:, xl, :, l, rows], relay.at[j, l, :, :, xl, a], sem1r.at[j, l]).start()

    def first_hop_send(j, tx, tl):
        rows = pl.ds(j * size, size)
        for a, ref in enumerate((mode, var)):
            remote(ref.at[:, tx, :, tl, rows], relay.at[j, l, :, :, xl, a], sem1.at[j], sem1r.at[j, l],
                   (z * NX * NY + tx * NY + y, tl)).start()

    def row_peer(i):
        return (xl + ROW_ORDER[i][0]) % NX, lax.rem(l + ROW_ORDER[i][1], n_lat)

    def first_hop_wait(j, source):
        pltpu.make_async_copy(relay.at[j, source], relay.at[j, source], sem1r.at[j, source]).wait()

    def plane_peer(i):
        tz = lax.rem(z + 3 * i, NZ)
        ty = lax.rem(y + i // NZ, NY)
        return tz, ty, (tz * NX * NY + xl * NY + ty, l)

    mine = pl.ds(plane * NX, NX)

    def second_hop_send(j, tz, ty):
        remote(relay.at[j, tz // 2, lax.rem(tz, 2), ty], buf.at[j, mine], sem2.at[0, j], sem2.at[1, j],
               (tz * NX * NY + xl * NY + ty, l)).start()

    def second_hop_opening(following):
        pairs = [(j, i) for j in following for i in range(n_row - 1)]
        for j in following:
            first_hop_own(j)
        for step, turn in enumerate(LAT_ORDER):
            source = lax.rem(l + n_lat - turn, n_lat)
            first_hop_wait(0, source)
            share = pairs[step * len(pairs) // n_lat : (step + 1) * len(pairs) // n_lat]
            for i in range(2 * NY):
                if i % 2 == 0 and i // 2 < len(share):
                    j, peer = share[i // 2]
                    first_hop_send(j, *row_peer(peer))
                tz, ty = 2 * source + i % 2, lax.rem(y + i // 2, NY)
                if i // 2 > 0:
                    second_hop_send(0, tz, ty)
                else:
                    @pl.when(tz != z)
                    def _():
                        second_hop_send(0, tz, ty)
        buf[0, mine] = relay[0, z // 2, lax.rem(z, 2), y]

    def second_hop(j, following):
        for f in following:
            first_hop_own(f)
        for source in range(n_lat):
            first_hop_wait(j, source)
        share = (n_plane - 1) // (n_row - 1)
        for i in range(n_row - 1):
            for f in following:
                first_hop_send(f, *row_peer(i))

            def body(k, carry):
                tz, ty, _ = plane_peer(k)
                second_hop_send(j, tz, ty)
                return carry

            lax.fori_loop(i * share + 1, n_plane if i == n_row - 2 else (i + 1) * share + 1, body, 0)
        buf[j, mine] = relay[j, z // 2, lax.rem(z, 2), y]

    for r in range(2):
        wpair[xl, r : r + 1, :] = jnp.full((1, LANES), weight[r], jnp.float32)

    barrier = pltpu.get_barrier_semaphore()

    def greet_plane(i, carry):
        pl.semaphore_signal(barrier, inc=1, device_id=plane_peer(i)[2], device_id_type=MESH)
        return carry

    lax.fori_loop(1, n_plane, greet_plane, 0)
    for i in range(n_row - 1):
        tx, tl = row_peer(i)
        pl.semaphore_signal(barrier, inc=1, device_id=(z * NX * NY + tx * NY + y, tl), device_id_type=MESH)
    first_hop_own(0)
    pl.semaphore_wait(barrier, n_plane + n_row - 2)

    for i in range(n_row - 1):
        first_hop_send(0, *row_peer(i))
    pair_copy = remote(wpair.at[xl], wpair.at[xl], wsem.at[0], wsem.at[1], (z * NX * NY + (1 - xl) * NY + y, l))
    pair_copy.start()

    def send_weights():
        pair_copy.wait()

        def body(i, carry):
            remote(wpair, wbuf.at[mine], wsem.at[2], wsem.at[3], plane_peer(i)[2]).start()
            return carry

        lax.fori_loop(1, n_plane, body, 0)
        wbuf[mine] = wpair[...]

    parity = lax.broadcasted_iota(jnp.int32, (8, LANES), 0)
    even = lax.rem(parity, 2) == 0
    zero = jnp.zeros((8, LANES), jnp.float32)

    def normalize_weights():
        pltpu.make_async_copy(wbuf.at[pl.ds(0, n_cfg - NX)], wbuf.at[pl.ds(0, n_cfg - NX)], wsem.at[3]).wait()

        def spread_weight(s, total):
            w = jnp.where(even, jnp.broadcast_to(wbuf[s, 0:1, :], (8, LANES)), jnp.broadcast_to(wbuf[s, 1:2, :], (8, LANES)))
            wnorm[s] = w
            return total + w

        total = pair_sum(lax.fori_loop(0, n_cfg, spread_weight, zero, unroll=8), even)

        def divide_weight(s, carry):
            wnorm[s] = wnorm[s] / total
            return carry

        lax.fori_loop(0, n_cfg, divide_weight, 0, unroll=8)

    def evaluate(j):
        pltpu.make_async_copy(buf.at[j, pl.ds(0, n_cfg - NX)], buf.at[j, pl.ds(0, n_cfg - NX)], sem2.at[1, j]).wait()

        def tile(q, carry):
            at = pl.ds(pl.multiple_of(q * 8, 8), 8)

            def first_moment(s, acc):
                return acc + wnorm[s] * buf[j, s, 0, at, :]

            centre = pair_sum(lax.fori_loop(0, n_cfg, first_moment, zero, unroll=8), even)

            def second_moment(s, acc):
                dev = buf[j, s, 0, at, :] - centre
                return acc + wnorm[s] * (buf[j, s, 1, at, :] + dev * dev)

            spread = jnp.sqrt(pair_sum(lax.fori_loop(0, n_cfg, second_moment, zero, unroll=8), even))

            def prepare(s, carry):
                root = lax.rsqrt(buf[j, s, 1, at, :])
                scale = root * math.sqrt(0.5 * LOG2E)
                coef[0, s] = scale * (centre - buf[j, s, 0, at, :])
                coef[1, s] = scale * spread
                coef[2, s] = wnorm[s] * root * (1.0 / math.sqrt(2.0 * math.pi))
                return carry

            lax.fori_loop(0, n_cfg, prepare, 0, unroll=8)

            column = (j * size + q * 8) * (LANES // 2)
            for t in range(4):
                lanes = pl.ds(pl.multiple_of(column + t * LANES, LANES), LANES)
                mom[0:1, lanes] = centre[2 * t : 2 * t + 1, :]
                mom[1:2, lanes] = spread[2 * t : 2 * t + 1, :]

            for base in range(0, dens.shape[0], GROUP):
                grid = [jnp.full((8, LANES), offset[base + g], jnp.float32) for g in range(GROUP)]

                def add_source(s, accs):
                    a, b, k = coef[0, s], coef[1, s], coef[2, s]
                    out = []
                    for g in range(GROUP):
                        x = a + grid[g] * b
                        out.append(accs[g] + k * jnp.exp2(-(x * x)))
                    return tuple(out)

                accs = lax.fori_loop(0, n_cfg, add_source, (zero,) * GROUP, unroll=2)
                for g in range(GROUP):
                    value = spread * pair_sum(accs[g], even)
                    for t in range(4):
                        lanes = pl.ds(pl.multiple_of(column + t * LANES, LANES), LANES)
                        dens[base + g : base + g + 1, lanes] = value[2 * t : 2 * t + 1, :]
            return carry

        lax.fori_loop(0, size // 8, tile, 0)

    def evaluate_step(j, carry):
        evaluate(j)
        return carry

    for j in range(CHUNKS):
        if j == 0:
            second_hop_opening(range(1, min(AHEAD, CHUNKS - 1) + 1))
        else:
            second_hop(j, [j + AHEAD] if j + AHEAD < CHUNKS else [])
        if j == 0:
            send_weights()
        if j == LAG - 1:
            normalize_weights()
        if j >= LAG:
            lax.fori_loop(j - LAG, j - LAG + 1, evaluate_step, 0)
    lax.fori_loop(CHUNKS - LAG, CHUNKS, evaluate_step, 0)

    def finish_first(i, carry):
        for j in range(CHUNKS):
            for a in range(2):
                pltpu.make_async_copy(relay.at[j, 0, :, :, 0, a], relay.at[j, 0, :, :, 0, a], sem1.at[j]).wait()
        return carry

    lax.fori_loop(1, n_row, finish_first, 0)
    for j in range(CHUNKS):
        pltpu.make_async_copy(buf.at[j, pl.ds(0, n_cfg - NX)], buf.at[j, pl.ds(0, n_cfg - NX)], sem2.at[0, j]).wait()

    pltpu.make_async_copy(wbuf.at[pl.ds(0, n_cfg - NX)], wbuf.at[pl.ds(0, n_cfg - NX)], wsem.at[2]).wait()


def per_device(latent_mode, latent_var, config_weight, grid_offset):
    n_cfg = lax.axis_size("cfg")
    n_lat = lax.axis_size("lat")
    own, width = latent_mode.shape
    grid = grid_offset.shape[0]
    lat_dev = width // n_cfg
    block = own * lat_dev // LANES
    size = block // CHUNKS

    def rows(a):
        a = a.reshape(own, width // LANES, LANES).transpose(1, 0, 2)
        return a.reshape(n_cfg // n_lat // (NX * NY), NX, NY, n_lat, block, LANES)

    vmem = pl.BlockSpec(memory_space=pltpu.VMEM)
    smem = pl.BlockSpec(memory_space=pltpu.SMEM)
    hbm = pl.BlockSpec(memory_space=pltpu.HBM)
    return pl.pallas_call(
        functools.partial(kernel, n_lat),
        out_shape=(
            jax.ShapeDtypeStruct((grid, lat_dev), jnp.float32),
            jax.ShapeDtypeStruct((2, lat_dev), jnp.float32),
        ),
        in_specs=[hbm, hbm, smem, smem],
        out_specs=(vmem, vmem),
        scratch_shapes=[
            pltpu.VMEM((CHUNKS, n_lat, NZ // n_lat, NY, NX, 2, size, LANES), jnp.float32),
            pltpu.VMEM((CHUNKS, n_cfg, 2, size, LANES), jnp.float32),
            pltpu.VMEM((NX, own, LANES), jnp.float32),
            pltpu.VMEM((n_cfg, own, LANES), jnp.float32),
            pltpu.VMEM((n_cfg, 8, LANES), jnp.float32),
            pltpu.VMEM((3, n_cfg, 8, LANES), jnp.float32),
            pltpu.SemaphoreType.DMA((CHUNKS,)),
            pltpu.SemaphoreType.DMA((CHUNKS, n_lat)),
            pltpu.SemaphoreType.DMA((2, CHUNKS)),
            pltpu.SemaphoreType.DMA((4,)),
        ],
        compiler_params=pltpu.CompilerParams(collective_id=0, has_side_effects=True, vmem_limit_bytes=52 * 1024 * 1024),
        name="mixture",
    )(rows(latent_mode), rows(latent_var), config_weight, grid_offset)


def solution(mesh):
    return jax.shard_map(
        per_device,
        mesh=mesh,
        in_specs=(P("cfg", "lat"), P("cfg", "lat"), P("cfg"), P()),
        out_specs=(P(None, ("cfg", "lat")), P(None, ("cfg", "lat"))),
        check_vma=False,
    )
```

```python
import functools
import math

import jax
import jax.numpy as jnp
from jax import lax
from jax.experimental import pallas as pl
from jax.experimental.pallas import tpu as pltpu
from jax.sharding import PartitionSpec as P

MESH = pl.DeviceIdType.MESH
LANES = 128
CHUNKS = 8
LAG = 2
AHEAD = 2
GROUP = 16
UNROLL = 4
MERGED = 5
DIST_ORDER = (4, 2, 6, 3, 5, 1, 7, 0)
LOG2E = 1.4426950408889634
NZ, NX, NY = 8, 2, 4
LAT_ORDER = (0, 2, 1, 3)
ROW_ORDER = ((1, 0), (0, 2), (1, 2), (0, 1), (1, 1), (0, 3), (1, 3))


def pair_sum(x, even):
    return x + jnp.where(even, pltpu.roll(x, 7, 0), pltpu.roll(x, 1, 0))


def kernel(n_lat, mode, var, weight, offset, dens, mom, relay, buf, wpair, wbuf, wnorm, wslot, coef, share_w, stat_own, stat_out, stat_in,
           line_own, line_out, line_in, part_out, part_in, sem1, sem1r, sem2, wsem, sem3):
    c = lax.axis_index("cfg")
    l = lax.axis_index("lat")
    z, xl, y = c // (NX * NY), (c // NY) % NX, c % NY
    n_row = NX * n_lat
    plane = z * NY + y
    n_plane = NZ * NY
    n_cfg = NZ * NX * NY
    size = buf.shape[3]

    def remote(src, dst, send, recv, device):
        return pltpu.make_async_remote_copy(
            src_ref=src, dst_ref=dst, send_sem=send, recv_sem=recv, device_id=device, device_id_type=MESH)

    def first_hop_own(j):
        rows = pl.ds(j * size, size)
        for a, ref in enumerate((mode, var)):
            pltpu.make_async_copy(ref.at[:, xl, :, l, rows], relay.at[j, l, :, :, xl, a], sem1r.at[j, l]).start()

    def first_hop_send(j, tx, tl):
        rows = pl.ds(j * size, size)
        for a, ref in enumerate((mode, var)):
            remote(ref.at[:, tx, :, tl, rows], relay.at[j, l, :, :, xl, a], sem1.at[j], sem1r.at[j, l],
                   (z * NX * NY + tx * NY + y, tl)).start()

    def row_peer(i):
        return (xl + ROW_ORDER[i][0]) % NX, lax.rem(l + ROW_ORDER[i][1], n_lat)

    def first_hop_wait(j, source):
        pltpu.make_async_copy(relay.at[j, source], relay.at[j, source], sem1r.at[j, source]).wait()

    def plane_peer(i):
        tz = lax.rem(z + 3 * i, NZ)
        ty = lax.rem(y + i // NZ, NY)
        return tz, ty, (tz * NX * NY + xl * NY + ty, l)

    mine = pl.ds(plane * NX, NX)

    def block(j, tz, ty):
        return relay.at[j, tz // 2, lax.rem(tz, 2), ty]

    def second_hop_send(j, tz, ty):
        if j >= MERGED:
            remote(block(j, tz, ty), buf.at[j, mine], sem2.at[0, j], sem2.at[1, j], (tz * NX * NY + xl * NY + ty, l)).start()

    odd = lax.rem(y, 2)

    def merge_route(d, dy):
        if d == 0:
            return z, y
        if d < 4:
            return lax.rem(z + NZ - d + 1, NZ), NY * d + y
        if d > 4:
            return lax.rem(z + NZ - d - 1, NZ), NY + 14 + NY * (NZ - d - 1) + y
        return lax.rem(z + 5 + 6 * (dy % 2), NZ), 16 + 14 * (dy % 2) + y // 2

    def merge_send(j, d, dy):
        to_z, slot = merge_route(d, dy)
        ty = lax.rem(y + dy, NY)
        src, dst = block(j, lax.rem(z + NZ - d, NZ), ty), buf.at[j, pl.ds(slot * NX, NX)]
        if dy == 0 and d in (0, 1, NZ - 1):
            dst[...] = src[...]
        else:
            remote(src, dst, sem2.at[0, j], sem2.at[1, j], (to_z * NX * NY + xl * NY + ty, l)).start()

    def merge_opening(source, half, dy):
        dz = 2 * source + half
        d = lax.rem(z + NZ - dz, NZ)
        up, down = jnp.logical_and(d >= 1, d <= 3), d >= 5
        slot = jnp.where(up, NY * d + y, jnp.where(down, NY + 14 + NY * (NZ - 1 - d) + y, jnp.where(d == 0, y, 16 + 14 * (dy % 2) + y // 2)))
        step = jnp.where(up, 1, jnp.where(down, NZ - 1, jnp.where(d == 0, 0, 1 + (NZ - 2) * (dy % 2))))
        to_z, ty = lax.rem(dz + step, NZ), lax.rem(y + dy, NY)
        src, dst = relay.at[0, source, half, ty], buf.at[0, pl.ds(slot * NX, NX)]

        def send():
            remote(src, dst, sem2.at[0, 0], sem2.at[1, 0], (to_z * NX * NY + xl * NY + ty, l)).start()

        if dy:
            send()
        else:
            pl.when(to_z != z)(send)

    def second_hop(j, following):
        pairs = [(f, i) for f in following for i in range(n_row - 1)]
        for f in following:
            first_hop_own(f)
        if j == 0:
            for step, turn in enumerate(LAT_ORDER):
                source = lax.rem(l + n_lat - turn, n_lat)
                first_hop_wait(0, source)
                for i in range(2 * NY):
                    merge_opening(source, i % 2, (i // 2 + 1) % NY)
                    if i % 2 == 1 and pairs:
                        f, peer = pairs.pop(0)
                        first_hop_send(f, *row_peer(peer))
            for d in (0, 1, NZ - 1):
                merge_send(0, d, 0)
            return
        for source in range(n_lat):
            first_hop_wait(j, source)
        if j < MERGED:
            for n, (dy, d) in enumerate((dy, d) for dy in range(NY) for d in DIST_ORDER):
                if n % 2 == 0 and n // 2 < len(pairs):
                    f, peer = pairs[n // 2]
                    first_hop_send(f, *row_peer(peer))
                merge_send(j, d, dy)
            return
        share = (n_plane - 1) // (n_row - 1)
        for i in range(n_row - 1):
            for f in following:
                first_hop_send(f, *row_peer(i))

            def body(k, carry):
                tz, ty, _ = plane_peer(k)
                second_hop_send(j, tz, ty)
                return carry

            lax.fori_loop(i * share + 1, n_plane if i == n_row - 2 else (i + 1) * share + 1, body, 0)
        buf[j, mine] = block(j, z, y)[...]

    for r in range(2):
        wpair[xl, r : r + 1, :] = jnp.full((1, LANES), weight[r], jnp.float32)

    barrier = pltpu.get_barrier_semaphore()

    def greet_plane(i, carry):
        pl.semaphore_signal(barrier, inc=1, device_id=plane_peer(i)[2], device_id_type=MESH)
        return carry

    lax.fori_loop(1, n_plane, greet_plane, 0)
    for i in range(n_row - 1):
        tx, tl = row_peer(i)
        pl.semaphore_signal(barrier, inc=1, device_id=(z * NX * NY + tx * NY + y, tl), device_id_type=MESH)
    first_hop_own(0)
    pl.semaphore_wait(barrier, n_plane + n_row - 2)

    for i in range(n_row - 1):
        first_hop_send(0, *row_peer(i))
    pair_copy = remote(wpair.at[xl], wpair.at[xl], wsem.at[0], wsem.at[1], (z * NX * NY + (1 - xl) * NY + y, l))
    pair_copy.start()

    def send_weights():
        pair_copy.wait()

        def body(i, carry):
            remote(wpair, wbuf.at[mine], wsem.at[2], wsem.at[3], plane_peer(i)[2]).start()
            return carry

        lax.fori_loop(1, n_plane, body, 0)
        wbuf[mine] = wpair[...]

    parity = lax.broadcasted_iota(jnp.int32, (8, LANES), 0)
    even = lax.rem(parity, 2) == 0
    zero = jnp.zeros((8, LANES), jnp.float32)

    def normalize_weights():
        pltpu.make_async_copy(wbuf.at[pl.ds(0, n_cfg - NX)], wbuf.at[pl.ds(0, n_cfg - NX)], wsem.at[3]).wait()

        def spread_weight(s, total):
            w = jnp.where(even, jnp.broadcast_to(wbuf[s, 0:1, :], (8, LANES)), jnp.broadcast_to(wbuf[s, 1:2, :], (8, LANES)))
            wnorm[s] = w
            return total + w

        total = pair_sum(lax.fori_loop(0, n_cfg, spread_weight, zero, unroll=8), even)

        def divide_weight(s, carry):
            wnorm[s] = wnorm[s] / total
            return carry

        lax.fori_loop(0, n_cfg, divide_weight, 0, unroll=8)

        def put(slot, plane_z, ys, carry=None):
            for i, yy in enumerate(ys):
                for a in range(NX):
                    wslot[(slot + i) * NX + a] = wnorm[(plane_z * NY + yy) * NX + a]

        def shifted(k):
            return lax.rem(z + NZ + k, NZ)

        put(0, z, range(NY))
        for d in range(1, 4):
            put(NY * d, shifted(d - 1), range(NY))
            put(NY + 14 + NY * (d - 1), shifted(1 - d), range(NY))
        put(16, shifted(3), (odd, odd + 2))
        put(30, shifted(-3), (1 - odd, 3 - odd))

        def weight_of(entries):
            acc = zero
            for plane_z, ys in entries:
                for yy in ys:
                    for a in range(NX):
                        acc = acc + wnorm[(plane_z * NY + yy) * NX + a]
            return pair_sum(acc, even)

        share_w[0] = weight_of([(z, range(NY))])
        share_w[1] = weight_of([(shifted(d), range(NY)) for d in range(1, 4)] + [(shifted(4), (odd, odd + 2))])
        share_w[2] = weight_of([(shifted(-d), range(NY)) for d in range(1, 4)] + [(shifted(4), (1 - odd, 3 - odd))])

    own_slots, far_slots = NX * NY, NX * 14

    def moments(j, w_ref, low, count):
        def first(s, acc):
            return acc[0] + w_ref[low + s] * buf[j, low + s, 0], acc[1] + w_ref[low + s]

        total, weight_sum = lax.fori_loop(0, count, first, (zero, zero), unroll=4)
        mean = pair_sum(total, even) / pair_sum(weight_sum, even)

        def second(s, acc):
            dev = buf[j, low + s, 0] - mean
            return acc + w_ref[low + s] * (buf[j, low + s, 1] + dev * dev)

        return mean, pair_sum(lax.fori_loop(0, count, second, zero, unroll=4), even)

    def accumulate(j, w_ref, low, count, unroll, centre, spread, store):
        def prepare(s, carry):
            var_s = buf[j, low + s, 1]
            coef[0, s] = (-0.5 * LOG2E) / var_s
            coef[1, s] = w_ref[low + s] * lax.rsqrt((2.0 * math.pi) * var_s)
            return carry

        lax.fori_loop(0, count, prepare, 0, unroll=4)

        for base in range(0, dens.shape[0], GROUP):
            points = [centre + offset[base + g] * spread for g in range(GROUP)]

            def add_source(s, accs):
                mean, rate, scale = buf[j, low + s, 0], coef[0, s], coef[1, s]
                out = []
                for g in range(GROUP):
                    gap = points[g] - mean
                    out.append(accs[g] + scale * jnp.exp2(gap * rate * gap))
                return tuple(out)

            accs = lax.fori_loop(0, count, add_source, (zero,) * GROUP, unroll=unroll)
            for g in range(GROUP):
                store(base + g, pair_sum(accs[g], even))

    tiles = 4
    width = tiles * LANES

    def put_rows(ref, row, column, value):
        for t in range(tiles):
            ref[row : row + 1, pl.ds(pl.multiple_of(column + t * LANES, LANES), LANES)] = value[2 * t : 2 * t + 1, :]

    def neighbour(side):
        return (lax.rem(z + NZ - 1 + 2 * side, NZ) * NX * NY + xl * NY + y, l)

    def received(ref, sem):
        pltpu.make_async_copy(ref, ref, sem).wait()

    def wait_blocks(j):
        count = n_cfg - NX * (3 if j < MERGED else 1)
        received(buf.at[j, pl.ds(0, count)], sem2.at[1, j])

    def send_stats(j):
        def side_stats(side, carry):
            mean, second = moments(j, wslot, own_slots + side * far_slots, far_slots)
            stat_out[j, side, 0] = mean
            stat_out[j, side, 1] = second
            return carry

        lax.fori_loop(0, 2, side_stats, 0)
        mean, second = moments(j, wslot, 0, own_slots)
        stat_own[j, 0] = mean
        stat_own[j, 1] = second
        for side in range(2):
            remote(stat_out.at[j, side], stat_in.at[j, side], sem3.at[0, j], sem3.at[1, j], neighbour(side)).start()

    def merge_stats(j):
        received(stat_in.at[j], sem3.at[1, j])
        means = [stat_own[j, 0], stat_in[j, 0, 0], stat_in[j, 1, 0]]
        seconds = [stat_own[j, 1], stat_in[j, 0, 1], stat_in[j, 1, 1]]
        shares = [share_w[i] for i in range(3)]
        centre = shares[0] * means[0] + shares[1] * means[1] + shares[2] * means[2]
        second = seconds[0] + seconds[1] + seconds[2]
        for share, mean in zip(shares, means):
            second = second + share * (mean - centre) * (mean - centre)
        spread = jnp.sqrt(second)
        for ref in (line_own.at[j], line_out.at[j]):
            ref[0] = centre
            ref[1] = spread
        put_rows(mom, 0, j * width, centre)
        put_rows(mom, 1, j * width, spread)
        for side in range(2):
            remote(line_out.at[j], line_in.at[j, 1 - side], sem3.at[2, j], sem3.at[3, j], neighbour(side)).start()

    def send_parts(j):
        received(line_in.at[j], sem3.at[3, j])

        def side_part(side, carry):
            def store(row, value):
                put_rows(part_out.at[j, side], row, 0, value)

            accumulate(j, wslot, own_slots + side * far_slots, far_slots, 7, line_in[j, side, 0], line_in[j, side, 1], store)
            return carry

        def send(side):
            remote(part_out.at[j, side], part_in.at[j, side], sem3.at[4, j], sem3.at[5, j], neighbour(side)).start()

        def store(row, value):
            put_rows(dens, row, j * width, value)

        lax.fori_loop(0, 2, side_part, 0)
        send(0)
        accumulate(j, wslot, 0, own_slots, 8, line_own[j, 0], line_own[j, 1], store)
        send(1)

    def add_parts(j):
        received(part_in.at[j], sem3.at[5, j])
        lanes = pl.ds(j * width, width)
        dens[:, lanes] = mom[1:2, lanes] * (dens[:, lanes] + part_in[j, 0] + part_in[j, 1])

    def evaluate(j):
        centre, second = moments(j, wnorm, 0, n_cfg)
        spread = jnp.sqrt(second)
        put_rows(mom, 0, j * width, centre)
        put_rows(mom, 1, j * width, spread)

        def store(row, value):
            put_rows(dens, row, j * width, spread * value)

        accumulate(j, wnorm, 0, n_cfg, 8, centre, spread, store)

    def ahead(j):
        return [j + AHEAD] if j + AHEAD < CHUNKS else []

    second_hop(0, range(1, AHEAD + 1))
    send_weights()
    second_hop(1, ahead(1))
    normalize_weights()
    for step in range(1, CHUNKS + 1):
        wait_blocks(step - 1)
        if step - 1 < MERGED:
            send_stats(step - 1)
        if 0 <= step - 2 < MERGED:
            merge_stats(step - 2)
        if step + 1 < CHUNKS:
            second_hop(step + 1, ahead(step + 1))
        if 0 <= step - 3 < MERGED:
            send_parts(step - 3)
        if step - 1 >= MERGED:
            evaluate(step - 1)
        if 0 <= step - 5 < MERGED:
            add_parts(step - 5)
    for j in range(CHUNKS - 4, MERGED):
        add_parts(j)

    def finish_first(i, carry):
        for j in range(CHUNKS):
            for a in range(2):
                pltpu.make_async_copy(relay.at[j, 0, :, :, 0, a], relay.at[j, 0, :, :, 0, a], sem1.at[j]).wait()
        return carry

    lax.fori_loop(1, n_row, finish_first, 0)
    for j in range(CHUNKS):
        count = n_cfg - NX * (3 if j < MERGED else 1)
        received(buf.at[j, pl.ds(0, count)], sem2.at[0, j])
    for j in range(MERGED):
        received(stat_out.at[j], sem3.at[0, j])
        received(line_in.at[j], sem3.at[2, j])
        received(part_out.at[j], sem3.at[4, j])

    pltpu.make_async_copy(wbuf.at[pl.ds(0, n_cfg - NX)], wbuf.at[pl.ds(0, n_cfg - NX)], wsem.at[2]).wait()


def per_device(latent_mode, latent_var, config_weight, grid_offset):
    n_cfg = lax.axis_size("cfg")
    n_lat = lax.axis_size("lat")
    own, width = latent_mode.shape
    grid = grid_offset.shape[0]
    lat_dev = width // n_cfg
    block = own * lat_dev // LANES
    size = block // CHUNKS

    def rows(a):
        a = a.reshape(own, width // LANES, LANES).transpose(1, 0, 2)
        return a.reshape(n_cfg // n_lat // (NX * NY), NX, NY, n_lat, block, LANES)

    vmem = pl.BlockSpec(memory_space=pltpu.VMEM)
    in_hbm = functools.partial(pltpu.with_memory_space_constraint, memory_space=pltpu.HBM)
    smem = pl.BlockSpec(memory_space=pltpu.SMEM)
    hbm = pl.BlockSpec(memory_space=pltpu.HBM)
    return pl.pallas_call(
        functools.partial(kernel, n_lat),
        out_shape=(
            jax.ShapeDtypeStruct((grid, lat_dev), jnp.float32),
            jax.ShapeDtypeStruct((2, lat_dev), jnp.float32),
        ),
        in_specs=[hbm, hbm, smem, smem],
        out_specs=(vmem, vmem),
        scratch_shapes=[
            pltpu.VMEM((CHUNKS, n_lat, NZ // n_lat, NY, NX, 2, size, LANES), jnp.float32),
            pltpu.VMEM((CHUNKS, n_cfg, 2, size, LANES), jnp.float32),
            pltpu.VMEM((NX, own, LANES), jnp.float32),
            pltpu.VMEM((n_cfg, own, LANES), jnp.float32),
            pltpu.VMEM((n_cfg, 8, LANES), jnp.float32),
            pltpu.VMEM((n_cfg, 8, LANES), jnp.float32),
            pltpu.VMEM((2, n_cfg, 8, LANES), jnp.float32),
            pltpu.VMEM((3, 8, LANES), jnp.float32),
            pltpu.VMEM((MERGED, 2, 8, LANES), jnp.float32),
            pltpu.VMEM((MERGED, 2, 2, 8, LANES), jnp.float32),
            pltpu.VMEM((MERGED, 2, 2, 8, LANES), jnp.float32),
            pltpu.VMEM((MERGED, 2, 8, LANES), jnp.float32),
            pltpu.VMEM((MERGED, 2, 8, LANES), jnp.float32),
            pltpu.VMEM((MERGED, 2, 2, 8, LANES), jnp.float32),
            pltpu.VMEM((MERGED, 2, grid, lat_dev // CHUNKS), jnp.float32),
            pltpu.VMEM((MERGED, 2, grid, lat_dev // CHUNKS), jnp.float32),
            pltpu.SemaphoreType.DMA((CHUNKS,)),
            pltpu.SemaphoreType.DMA((CHUNKS, n_lat)),
            pltpu.SemaphoreType.DMA((2, CHUNKS)),
            pltpu.SemaphoreType.DMA((4,)),
            pltpu.SemaphoreType.DMA((6, MERGED)),
        ],
        compiler_params=pltpu.CompilerParams(collective_id=0, has_side_effects=True, vmem_limit_bytes=52 * 1024 * 1024),
        name="mixture",
    )(rows(latent_mode), rows(latent_var), in_hbm(config_weight), in_hbm(grid_offset))


def solution(mesh):
    return jax.shard_map(
        per_device,
        mesh=mesh,
        in_specs=(P("cfg", "lat"), P("cfg", "lat"), P("cfg"), P()),
        out_specs=(P(None, ("cfg", "lat")), P(None, ("cfg", "lat"))),
        check_vma=False,
    )
```

```python
import functools
import math

import jax
import jax.numpy as jnp
from jax import lax
from jax.experimental import pallas as pl
from jax.experimental.pallas import tpu as pltpu
from jax.sharding import PartitionSpec as P

MESH = pl.DeviceIdType.MESH
LANES = 128
CHUNKS = 8
LAG = 2
AHEAD = 2
GROUP = 16
UNROLL = 4
MERGED = 5
DIST_ORDER = (4, 3, 5, 2, 6, 1, 7, 0)
LOG2E = 1.4426950408889634
NZ, NX, NY = 8, 2, 4
LAT_ORDER = (0, 2, 1, 3)
ROW_ORDER = ((1, 0), (0, 2), (1, 2), (0, 1), (1, 1), (0, 3), (1, 3))


def pair_sum(x, even):
    return x + jnp.where(even, pltpu.roll(x, 7, 0), pltpu.roll(x, 1, 0))


def kernel(n_lat, mode, var, weight_hbm, offset_hbm, dens, mom, weight, offset, small_sem, relay, buf, wpair, wbuf, wnorm, wslot, coef, share_w, stat_own, stat_out, stat_in,
           line_own, line_out, line_in, part_out, part_in, sem1, sem1r, sem2, wsem, sem3):
    c = lax.axis_index("cfg")
    l = lax.axis_index("lat")
    z, xl, y = c // (NX * NY), (c // NY) % NX, c % NY
    n_row = NX * n_lat
    plane = z * NY + y
    n_plane = NZ * NY
    n_cfg = NZ * NX * NY
    size = buf.shape[3]

    def remote(src, dst, send, recv, device):
        return pltpu.make_async_remote_copy(
            src_ref=src, dst_ref=dst, send_sem=send, recv_sem=recv, device_id=device, device_id_type=MESH)

    def first_hop_own(j):
        rows = pl.ds(j * size, size)
        for a, ref in enumerate((mode, var)):
            pltpu.make_async_copy(ref.at[:, xl, :, l, rows], relay.at[j, l, :, :, xl, a], sem1r.at[j, l]).start()

    def first_hop_send(j, tx, tl):
        rows = pl.ds(j * size, size)
        for a, ref in enumerate((mode, var)):
            remote(ref.at[:, tx, :, tl, rows], relay.at[j, l, :, :, xl, a], sem1.at[j], sem1r.at[j, l],
                   (z * NX * NY + tx * NY + y, tl)).start()

    def row_peer(i):
        return (xl + ROW_ORDER[i][0]) % NX, lax.rem(l + ROW_ORDER[i][1], n_lat)

    def first_hop_wait(j, source):
        pltpu.make_async_copy(relay.at[j, source], relay.at[j, source], sem1r.at[j, source]).wait()

    def plane_peer(i):
        tz = lax.rem(z + 3 * i, NZ)
        ty = lax.rem(y + i // NZ, NY)
        return tz, ty, (tz * NX * NY + xl * NY + ty, l)

    mine = pl.ds(plane * NX, NX)

    def block(j, tz, ty):
        return relay.at[j, tz // 2, lax.rem(tz, 2), ty]

    def second_hop_send(j, tz, ty):
        if j >= MERGED:
            remote(block(j, tz, ty), buf.at[j, mine], sem2.at[0, j], sem2.at[1, j], (tz * NX * NY + xl * NY + ty, l)).start()

    odd = lax.rem(y, 2)

    def merge_route(d, dy):
        if d == 0:
            return z, y
        if d < 4:
            return lax.rem(z + NZ - d + 1, NZ), NY * d + y
        if d > 4:
            return lax.rem(z + NZ - d - 1, NZ), NY + 14 + NY * (NZ - d - 1) + y
        return lax.rem(z + 5 + 6 * (dy % 2), NZ), 16 + 14 * (dy % 2) + y // 2

    def merge_send(j, d, dy):
        to_z, slot = merge_route(d, dy)
        ty = lax.rem(y + dy, NY)
        src, dst = block(j, lax.rem(z + NZ - d, NZ), ty), buf.at[j, pl.ds(slot * NX, NX)]
        if dy == 0 and d in (0, 1, NZ - 1):
            dst[...] = src[...]
        else:
            remote(src, dst, sem2.at[0, j], sem2.at[1, j], (to_z * NX * NY + xl * NY + ty, l)).start()

    def merge_opening(source, half, dy):
        dz = 2 * source + half
        d = lax.rem(z + NZ - dz, NZ)
        up, down = jnp.logical_and(d >= 1, d <= 3), d >= 5
        slot = jnp.where(up, NY * d + y, jnp.where(down, NY + 14 + NY * (NZ - 1 - d) + y, jnp.where(d == 0, y, 16 + 14 * (dy % 2) + y // 2)))
        step = jnp.where(up, 1, jnp.where(down, NZ - 1, jnp.where(d == 0, 0, 1 + (NZ - 2) * (dy % 2))))
        to_z, ty = lax.rem(dz + step, NZ), lax.rem(y + dy, NY)
        src, dst = relay.at[0, source, half, ty], buf.at[0, pl.ds(slot * NX, NX)]

        def send():
            remote(src, dst, sem2.at[0, 0], sem2.at[1, 0], (to_z * NX * NY + xl * NY + ty, l)).start()

        if dy:
            send()
        else:
            pl.when(to_z != z)(send)

    def second_hop(j, following):
        pairs = [(f, i) for f in following for i in range(n_row - 1)]
        for f in following:
            first_hop_own(f)
        if j == 0:
            for step, turn in enumerate(LAT_ORDER):
                source = lax.rem(l + n_lat - turn, n_lat)
                first_hop_wait(0, source)
                for i in range(2 * NY):
                    merge_opening(source, i % 2, (i // 2 + 1) % NY)
                    if i % 2 == 1 and pairs:
                        f, peer = pairs.pop(0)
                        first_hop_send(f, *row_peer(peer))
            for d in (0, 1, NZ - 1):
                merge_send(0, d, 0)
            return
        for source in range(n_lat):
            first_hop_wait(j, source)
        if j < MERGED:
            for n, (dy, d) in enumerate((dy, d) for dy in range(NY) for d in DIST_ORDER):
                if n % 2 == 0 and n // 2 < len(pairs):
                    f, peer = pairs[n // 2]
                    first_hop_send(f, *row_peer(peer))
                merge_send(j, d, dy)
            return
        for n, (dy, d) in enumerate((dy, d) for dy in range(NY) for d in DIST_ORDER):
            if n % 2 == 0 and n // 2 < len(pairs):
                f, peer = pairs[n // 2]
                first_hop_send(f, *row_peer(peer))
            if (dy, d) != (0, 0):
                second_hop_send(j, lax.rem(z + NZ - d, NZ), lax.rem(y + dy, NY))
        buf[j, mine] = block(j, z, y)[...]

    small = [pltpu.make_async_copy(weight_hbm, weight, small_sem.at[0]), pltpu.make_async_copy(offset_hbm, offset, small_sem.at[1])]
    for copy in small:
        copy.start()

    barrier = pltpu.get_barrier_semaphore()

    def greet_plane(i, carry):
        pl.semaphore_signal(barrier, inc=1, device_id=plane_peer(i)[2], device_id_type=MESH)
        return carry

    lax.fori_loop(1, n_plane, greet_plane, 0)
    for i in range(n_row - 1):
        tx, tl = row_peer(i)
        pl.semaphore_signal(barrier, inc=1, device_id=(z * NX * NY + tx * NY + y, tl), device_id_type=MESH)
    first_hop_own(0)
    for copy in small:
        copy.wait()
    for r in range(2):
        wpair[xl, r : r + 1, :] = jnp.full((1, LANES), weight[r], jnp.float32)
    pl.semaphore_wait(barrier, n_plane + n_row - 2)

    for i in range(n_row - 1):
        first_hop_send(0, *row_peer(i))
    pair_copy = remote(wpair.at[xl], wpair.at[xl], wsem.at[0], wsem.at[1], (z * NX * NY + (1 - xl) * NY + y, l))
    pair_copy.start()

    def send_weights():
        pair_copy.wait()

        def body(i, carry):
            remote(wpair, wbuf.at[mine], wsem.at[2], wsem.at[3], plane_peer(i)[2]).start()
            return carry

        lax.fori_loop(1, n_plane, body, 0)
        wbuf[mine] = wpair[...]

    parity = lax.broadcasted_iota(jnp.int32, (8, LANES), 0)
    even = lax.rem(parity, 2) == 0
    zero = jnp.zeros((8, LANES), jnp.float32)

    def normalize_weights():
        pltpu.make_async_copy(wbuf.at[pl.ds(0, n_cfg - NX)], wbuf.at[pl.ds(0, n_cfg - NX)], wsem.at[3]).wait()

        def spread_weight(s, total):
            w = jnp.where(even, jnp.broadcast_to(wbuf[s, 0:1, :], (8, LANES)), jnp.broadcast_to(wbuf[s, 1:2, :], (8, LANES)))
            wnorm[s] = w
            return total + w

        total = pair_sum(lax.fori_loop(0, n_cfg, spread_weight, zero, unroll=8), even)

        def divide_weight(s, carry):
            wnorm[s] = wnorm[s] / total
            return carry

        lax.fori_loop(0, n_cfg, divide_weight, 0, unroll=8)

        def put(slot, plane_z, ys, carry=None):
            for i, yy in enumerate(ys):
                for a in range(NX):
                    wslot[(slot + i) * NX + a] = wnorm[(plane_z * NY + yy) * NX + a]

        def shifted(k):
            return lax.rem(z + NZ + k, NZ)

        put(0, z, range(NY))
        for d in range(1, 4):
            put(NY * d, shifted(d - 1), range(NY))
            put(NY + 14 + NY * (d - 1), shifted(1 - d), range(NY))
        put(16, shifted(3), (odd, odd + 2))
        put(30, shifted(-3), (1 - odd, 3 - odd))

        def weight_of(entries):
            acc = zero
            for plane_z, ys in entries:
                for yy in ys:
                    for a in range(NX):
                        acc = acc + wnorm[(plane_z * NY + yy) * NX + a]
            return pair_sum(acc, even)

        share_w[0] = weight_of([(z, range(NY))])
        share_w[1] = weight_of([(shifted(d), range(NY)) for d in range(1, 4)] + [(shifted(4), (odd, odd + 2))])
        share_w[2] = weight_of([(shifted(-d), range(NY)) for d in range(1, 4)] + [(shifted(4), (1 - odd, 3 - odd))])

    own_slots, far_slots = NX * NY, NX * 14

    def moments(j, w_ref, low, count):
        def first(s, acc):
            return acc[0] + w_ref[low + s] * buf[j, low + s, 0], acc[1] + w_ref[low + s]

        total, weight_sum = lax.fori_loop(0, count, first, (zero, zero), unroll=True if count == 8 else 14 if count == 28 else 16)
        mean = pair_sum(total, even) / pair_sum(weight_sum, even)

        def second(s, acc):
            dev = buf[j, low + s, 0] - mean
            return acc + w_ref[low + s] * (buf[j, low + s, 1] + dev * dev)

        return mean, pair_sum(lax.fori_loop(0, count, second, zero, unroll=True if count == 8 else 14 if count == 28 else 16), even)

    def accumulate(j, w_ref, low, count, unroll, centre, spread, store):
        def prepare(s, carry):
            var_s = buf[j, low + s, 1]
            coef[0, s] = (-0.5 * LOG2E) / var_s
            coef[1, s] = w_ref[low + s] * lax.rsqrt((2.0 * math.pi) * var_s)
            return carry

        lax.fori_loop(0, count, prepare, 0, unroll=True if count == 8 else 7 if count == 28 else 16)

        for base in range(0, dens.shape[0], GROUP):
            points = [centre + offset[base + g] * spread for g in range(GROUP)]

            def add_source(s, accs):
                mean, rate, scale = buf[j, low + s, 0], coef[0, s], coef[1, s]
                out = []
                for g in range(GROUP):
                    gap = points[g] - mean
                    out.append(accs[g] + scale * jnp.exp2(gap * rate * gap))
                return tuple(out)

            accs = lax.fori_loop(0, count, add_source, (zero,) * GROUP, unroll=unroll)
            for g in range(GROUP):
                store(base + g, pair_sum(accs[g], even))

    def unpaired(x):
        return jnp.where(even, x, pltpu.roll(x, 1, 0)), jnp.where(even, pltpu.roll(x, 7, 0), x)

    tiles = 4
    width = tiles * LANES

    def put_rows(ref, row, column, value):
        for t in range(tiles):
            ref[row : row + 1, pl.ds(pl.multiple_of(column + t * LANES, LANES), LANES)] = value[2 * t : 2 * t + 1, :]

    def neighbour(side):
        return (lax.rem(z + NZ - 1 + 2 * side, NZ) * NX * NY + xl * NY + y, l)

    def received(ref, sem):
        pltpu.make_async_copy(ref, ref, sem).wait()

    def wait_blocks(j):
        count = n_cfg - NX * (3 if j < MERGED else 1)
        received(buf.at[j, pl.ds(0, count)], sem2.at[1, j])

    def send_stats(j):
        def side_stats(side, carry):
            mean, second = moments(j, wslot, own_slots + side * far_slots, far_slots)
            stat_out[j, side] = jnp.where(even, mean, second)
            return carry

        lax.fori_loop(0, 2, side_stats, 0)
        mean, second = moments(j, wslot, 0, own_slots)
        stat_own[j, 0] = mean
        stat_own[j, 1] = second
        for side in range(2):
            remote(stat_out.at[j, side], stat_in.at[j, side], sem3.at[0, j], sem3.at[1, j], neighbour(side)).start()

    def merge_stats(j):
        received(stat_in.at[j], sem3.at[1, j])
        pairs = [unpaired(stat_in[j, side]) for side in range(2)]
        means = [stat_own[j, 0]] + [p[0] for p in pairs]
        seconds = [stat_own[j, 1]] + [p[1] for p in pairs]
        shares = [share_w[i] for i in range(3)]
        centre = shares[0] * means[0] + shares[1] * means[1] + shares[2] * means[2]
        second = seconds[0] + seconds[1] + seconds[2]
        for share, mean in zip(shares, means):
            second = second + share * (mean - centre) * (mean - centre)
        spread = jnp.sqrt(second)
        line_out[j] = jnp.where(even, centre, spread)
        line_own[j, 0] = centre
        line_own[j, 1] = spread
        put_rows(mom, 0, j * width, centre)
        put_rows(mom, 1, j * width, spread)
        for side in range(2):
            remote(line_out.at[j], line_in.at[j, 1 - side], sem3.at[2, j], sem3.at[3, j], neighbour(side)).start()

    def send_parts(j):
        received(line_in.at[j], sem3.at[3, j])

        def side_part(side, carry):
            def store(row, value):
                put_rows(part_out.at[j, side], row, 0, value)

            accumulate(j, wslot, own_slots + side * far_slots, far_slots, 7, *unpaired(line_in[j, side]), store)
            return carry

        def send(side):
            remote(part_out.at[j, side], part_in.at[j, side], sem3.at[4, j], sem3.at[5, j], neighbour(side)).start()

        def store(row, value):
            put_rows(dens, row, j * width, value)

        lax.fori_loop(0, 2, side_part, 0)
        send(0)
        accumulate(j, wslot, 0, own_slots, 8, line_own[j, 0], line_own[j, 1], store)
        send(1)

    def add_parts(j):
        received(part_in.at[j], sem3.at[5, j])
        lanes = pl.ds(j * width, width)
        dens[:, lanes] = mom[1:2, lanes] * (dens[:, lanes] + part_in[j, 0] + part_in[j, 1])

    def evaluate(j):
        centre, second = moments(j, wnorm, 0, n_cfg)
        spread = jnp.sqrt(second)
        put_rows(mom, 0, j * width, centre)
        put_rows(mom, 1, j * width, spread)

        def store(row, value):
            put_rows(dens, row, j * width, spread * value)

        accumulate(j, wnorm, 0, n_cfg, 8, centre, spread, store)

    def ahead(j):
        return [j + AHEAD] if j + AHEAD < CHUNKS else []

    second_hop(0, range(1, AHEAD + 1))
    send_weights()
    second_hop(1, ahead(1))
    normalize_weights()
    for step in range(1, CHUNKS + 1):
        wait_blocks(step - 1)
        if step - 1 < MERGED:
            send_stats(step - 1)
        if 0 <= step - 2 < MERGED:
            merge_stats(step - 2)
        if step + 1 < CHUNKS:
            second_hop(step + 1, ahead(step + 1))
        if 0 <= step - 3 < MERGED:
            send_parts(step - 3)
        if step - 1 >= MERGED:
            evaluate(step - 1)
        if 0 <= step - 5 < MERGED:
            add_parts(step - 5)
    for j in range(CHUNKS - 4, MERGED):
        add_parts(j)

    def finish_first(i, carry):
        for j in range(CHUNKS):
            for a in range(2):
                pltpu.make_async_copy(relay.at[j, 0, :, :, 0, a], relay.at[j, 0, :, :, 0, a], sem1.at[j]).wait()
        return carry

    lax.fori_loop(1, n_row, finish_first, 0)
    for j in range(CHUNKS):
        count = n_cfg - NX * (3 if j < MERGED else 1)
        received(buf.at[j, pl.ds(0, count)], sem2.at[0, j])
    for j in range(MERGED):
        received(stat_out.at[j], sem3.at[0, j])
        received(line_in.at[j], sem3.at[2, j])
        received(part_out.at[j], sem3.at[4, j])

    pltpu.make_async_copy(wbuf.at[pl.ds(0, n_cfg - NX)], wbuf.at[pl.ds(0, n_cfg - NX)], wsem.at[2]).wait()


def per_device(latent_mode, latent_var, config_weight, grid_offset):
    n_cfg = lax.axis_size("cfg")
    n_lat = lax.axis_size("lat")
    own, width = latent_mode.shape
    grid = grid_offset.shape[0]
    lat_dev = width // n_cfg
    block = own * lat_dev // LANES
    size = block // CHUNKS

    def rows(a):
        a = a.reshape(own, width // LANES, LANES).transpose(1, 0, 2)
        return a.reshape(n_cfg // n_lat // (NX * NY), NX, NY, n_lat, block, LANES)

    vmem = pl.BlockSpec(memory_space=pltpu.VMEM)
    in_hbm = functools.partial(pltpu.with_memory_space_constraint, memory_space=pltpu.HBM)
    hbm = pl.BlockSpec(memory_space=pltpu.HBM)
    return pl.pallas_call(
        functools.partial(kernel, n_lat),
        out_shape=(
            jax.ShapeDtypeStruct((grid, lat_dev), jnp.float32),
            jax.ShapeDtypeStruct((2, lat_dev), jnp.float32),
        ),
        in_specs=[hbm, hbm, hbm, hbm],
        out_specs=(vmem, vmem),
        scratch_shapes=[
            pltpu.SMEM((own,), jnp.float32),
            pltpu.SMEM((grid,), jnp.float32),
            pltpu.SemaphoreType.DMA((2,)),
            pltpu.VMEM((CHUNKS, n_lat, NZ // n_lat, NY, NX, 2, size, LANES), jnp.float32),
            pltpu.VMEM((CHUNKS, n_cfg, 2, size, LANES), jnp.float32),
            pltpu.VMEM((NX, own, LANES), jnp.float32),
            pltpu.VMEM((n_cfg, own, LANES), jnp.float32),
            pltpu.VMEM((n_cfg, 8, LANES), jnp.float32),
            pltpu.VMEM((n_cfg, 8, LANES), jnp.float32),
            pltpu.VMEM((2, n_cfg, 8, LANES), jnp.float32),
            pltpu.VMEM((3, 8, LANES), jnp.float32),
            pltpu.VMEM((MERGED, 2, 8, LANES), jnp.float32),
            pltpu.VMEM((MERGED, 2, 8, LANES), jnp.float32),
            pltpu.VMEM((MERGED, 2, 8, LANES), jnp.float32),
            pltpu.VMEM((MERGED, 2, 8, LANES), jnp.float32),
            pltpu.VMEM((MERGED, 8, LANES), jnp.float32),
            pltpu.VMEM((MERGED, 2, 8, LANES), jnp.float32),
            pltpu.VMEM((MERGED, 2, grid, lat_dev // CHUNKS), jnp.float32),
            pltpu.VMEM((MERGED, 2, grid, lat_dev // CHUNKS), jnp.float32),
            pltpu.SemaphoreType.DMA((CHUNKS,)),
            pltpu.SemaphoreType.DMA((CHUNKS, n_lat)),
            pltpu.SemaphoreType.DMA((2, CHUNKS)),
            pltpu.SemaphoreType.DMA((4,)),
            pltpu.SemaphoreType.DMA((6, MERGED)),
        ],
        compiler_params=pltpu.CompilerParams(collective_id=0, has_side_effects=True, vmem_limit_bytes=52 * 1024 * 1024),
        name="mixture",
    )(rows(latent_mode), rows(latent_var), in_hbm(config_weight), in_hbm(grid_offset))


def solution(mesh):
    return jax.shard_map(
        per_device,
        mesh=mesh,
        in_specs=(P("cfg", "lat"), P("cfg", "lat"), P("cfg"), P()),
        out_specs=(P(None, ("cfg", "lat")), P(None, ("cfg", "lat"))),
        check_vma=False,
    )
```

```python
import functools
import math

import jax
import jax.numpy as jnp
from jax import lax
from jax.experimental import pallas as pl
from jax.experimental.pallas import tpu as pltpu
from jax.sharding import PartitionSpec as P

MESH = pl.DeviceIdType.MESH
LANES = 128
CHUNKS = 8
LAG = 2
AHEAD = 2
GROUP = 16
UNROLL = 4
MERGED = 5
DIST_ORDER = (4, 3, 5, 2, 6, 1, 7, 0)
LOG2E = 1.4426950408889634
NZ, NX, NY = 8, 2, 4
LAT_ORDER = (0, 2, 1, 3)
ROW_ORDER = ((1, 0), (0, 2), (1, 2), (0, 1), (1, 1), (0, 3), (1, 3))


def pair_sum(x, even):
    return x + jnp.where(even, pltpu.roll(x, 7, 0), pltpu.roll(x, 1, 0))


def kernel(n_lat, mode, var, weight_hbm, offset_hbm, dens, mom, weight, offset, small_sem, relay, buf, wpair, wbuf, wnorm, wslot, coef, share_w, stat_own, stat_out, stat_in,
           line_own, line_out, line_in, part_out, part_in, sem1, sem1r, sem2, wsem, sem3):
    c = lax.axis_index("cfg")
    l = lax.axis_index("lat")
    z, xl, y = c // (NX * NY), (c // NY) % NX, c % NY
    n_row = NX * n_lat
    plane = z * NY + y
    n_plane = NZ * NY
    n_cfg = NZ * NX * NY
    size = buf.shape[3]

    def remote(src, dst, send, recv, device):
        return pltpu.make_async_remote_copy(
            src_ref=src, dst_ref=dst, send_sem=send, recv_sem=recv, device_id=device, device_id_type=MESH)

    def first_hop_own(j):
        rows = pl.ds(j * size, size)
        for a, ref in enumerate((mode, var)):
            pltpu.make_async_copy(ref.at[:, xl, :, l, rows], relay.at[j, l, :, :, xl, a], sem1r.at[j, l]).start()

    def first_hop_send(j, tx, tl):
        rows = pl.ds(j * size, size)
        for a, ref in enumerate((mode, var)):
            remote(ref.at[:, tx, :, tl, rows], relay.at[j, l, :, :, xl, a], sem1.at[j], sem1r.at[j, l],
                   (z * NX * NY + tx * NY + y, tl)).start()

    def row_peer(i):
        return (xl + ROW_ORDER[i][0]) % NX, lax.rem(l + ROW_ORDER[i][1], n_lat)

    def first_hop_wait(j, source):
        pltpu.make_async_copy(relay.at[j, source], relay.at[j, source], sem1r.at[j, source]).wait()

    def plane_peer(i):
        tz = lax.rem(z + 3 * i, NZ)
        ty = lax.rem(y + i // NZ, NY)
        return tz, ty, (tz * NX * NY + xl * NY + ty, l)

    mine = pl.ds(plane * NX, NX)

    def block(j, tz, ty):
        return relay.at[j, tz // 2, lax.rem(tz, 2), ty]

    def second_hop_send(j, tz, ty):
        if j >= MERGED:
            remote(block(j, tz, ty), buf.at[j, mine], sem2.at[0, j], sem2.at[1, j], (tz * NX * NY + xl * NY + ty, l)).start()

    odd = lax.rem(y, 2)

    def merge_route(d, dy):
        if d == 0:
            return z, y
        if d < 4:
            return lax.rem(z + NZ - d + 1, NZ), NY * d + y
        if d > 4:
            return lax.rem(z + NZ - d - 1, NZ), NY + 14 + NY * (NZ - d - 1) + y
        return lax.rem(z + 5 + 6 * (dy % 2), NZ), 16 + 14 * (dy % 2) + y // 2

    def merge_send(j, d, dy):
        to_z, slot = merge_route(d, dy)
        ty = lax.rem(y + dy, NY)
        src, dst = block(j, lax.rem(z + NZ - d, NZ), ty), buf.at[j, pl.ds(slot * NX, NX)]
        if dy == 0 and d in (0, 1, NZ - 1):
            dst[...] = src[...]
        else:
            remote(src, dst, sem2.at[0, j], sem2.at[1, j], (to_z * NX * NY + xl * NY + ty, l)).start()

    def merge_opening(source, half, dy):
        dz = 2 * source + half
        d = lax.rem(z + NZ - dz, NZ)
        up, down = jnp.logical_and(d >= 1, d <= 3), d >= 5
        slot = jnp.where(up, NY * d + y, jnp.where(down, NY + 14 + NY * (NZ - 1 - d) + y, jnp.where(d == 0, y, 16 + 14 * (dy % 2) + y // 2)))
        step = jnp.where(up, 1, jnp.where(down, NZ - 1, jnp.where(d == 0, 0, 1 + (NZ - 2) * (dy % 2))))
        to_z, ty = lax.rem(dz + step, NZ), lax.rem(y + dy, NY)
        src, dst = relay.at[0, source, half, ty], buf.at[0, pl.ds(slot * NX, NX)]

        def send():
            remote(src, dst, sem2.at[0, 0], sem2.at[1, 0], (to_z * NX * NY + xl * NY + ty, l)).start()

        if dy:
            send()
        else:
            pl.when(to_z != z)(send)

    def second_hop(j, following):
        pairs = [(f, i) for f in following for i in range(n_row - 1)]
        for f in following:
            first_hop_own(f)
        if j == 0:
            for step, turn in enumerate(LAT_ORDER):
                source = lax.rem(l + n_lat - turn, n_lat)
                first_hop_wait(0, source)
                for i in range(2 * NY):
                    merge_opening(source, i % 2, (i // 2 + 1) % NY)
                    if i % 2 == 1 and pairs:
                        f, peer = pairs.pop(0)
                        first_hop_send(f, *row_peer(peer))
            for d in (0, 1, NZ - 1):
                merge_send(0, d, 0)
            return
        for source in range(n_lat):
            first_hop_wait(j, source)
        if j < MERGED:
            for n, (dy, d) in enumerate((dy, d) for dy in range(NY) for d in DIST_ORDER):
                if n % 2 == 0 and n // 2 < len(pairs):
                    f, peer = pairs[n // 2]
                    first_hop_send(f, *row_peer(peer))
                merge_send(j, d, dy)
            return
        for n, (dy, d) in enumerate((dy, d) for dy in range(NY) for d in DIST_ORDER):
            if n % 2 == 0 and n // 2 < len(pairs):
                f, peer = pairs[n // 2]
                first_hop_send(f, *row_peer(peer))
            if (dy, d) != (0, 0):
                second_hop_send(j, lax.rem(z + NZ - d, NZ), lax.rem(y + dy, NY))
        buf[j, mine] = block(j, z, y)[...]

    small = [pltpu.make_async_copy(weight_hbm, weight, small_sem.at[0]), pltpu.make_async_copy(offset_hbm, offset, small_sem.at[1])]
    for copy in small:
        copy.start()

    barrier = pltpu.get_barrier_semaphore()

    def greet_plane(i, carry):
        pl.semaphore_signal(barrier, inc=1, device_id=plane_peer(i)[2], device_id_type=MESH)
        return carry

    lax.fori_loop(1, n_plane, greet_plane, 0)
    for i in range(n_row - 1):
        tx, tl = row_peer(i)
        pl.semaphore_signal(barrier, inc=1, device_id=(z * NX * NY + tx * NY + y, tl), device_id_type=MESH)
    first_hop_own(0)
    for copy in small:
        copy.wait()
    for r in range(2):
        wpair[xl, r : r + 1, :] = jnp.full((1, LANES), weight[r], jnp.float32)
    pl.semaphore_wait(barrier, n_plane + n_row - 2)

    for i in range(n_row - 1):
        first_hop_send(0, *row_peer(i))
    pair_copy = remote(wpair.at[xl], wpair.at[xl], wsem.at[0], wsem.at[1], (z * NX * NY + (1 - xl) * NY + y, l))
    pair_copy.start()

    def send_weights():
        pair_copy.wait()

        def body(i, carry):
            remote(wpair, wbuf.at[mine], wsem.at[2], wsem.at[3], plane_peer(i)[2]).start()
            return carry

        lax.fori_loop(1, n_plane, body, 0)
        wbuf[mine] = wpair[...]

    parity = lax.broadcasted_iota(jnp.int32, (8, LANES), 0)
    even = lax.rem(parity, 2) == 0
    zero = jnp.zeros((8, LANES), jnp.float32)

    def normalize_weights():
        pltpu.make_async_copy(wbuf.at[pl.ds(0, n_cfg - NX)], wbuf.at[pl.ds(0, n_cfg - NX)], wsem.at[3]).wait()

        def spread_weight(s, total):
            w = jnp.where(even, jnp.broadcast_to(wbuf[s, 0:1, :], (8, LANES)), jnp.broadcast_to(wbuf[s, 1:2, :], (8, LANES)))
            wnorm[s] = w
            return total + w

        total = pair_sum(lax.fori_loop(0, n_cfg, spread_weight, zero, unroll=8), even)

        def divide_weight(s, carry):
            wnorm[s] = wnorm[s] / total
            return carry

        lax.fori_loop(0, n_cfg, divide_weight, 0, unroll=8)

        def put(slot, plane_z, ys, carry=None):
            for i, yy in enumerate(ys):
                for a in range(NX):
                    wslot[(slot + i) * NX + a] = wnorm[(plane_z * NY + yy) * NX + a]

        def shifted(k):
            return lax.rem(z + NZ + k, NZ)

        put(0, z, range(NY))
        for d in range(1, 4):
            put(NY * d, shifted(d - 1), range(NY))
            put(NY + 14 + NY * (d - 1), shifted(1 - d), range(NY))
        put(16, shifted(3), (odd, odd + 2))
        put(30, shifted(-3), (1 - odd, 3 - odd))

        def weight_of(entries):
            acc = zero
            for plane_z, ys in entries:
                for yy in ys:
                    for a in range(NX):
                        acc = acc + wnorm[(plane_z * NY + yy) * NX + a]
            return pair_sum(acc, even)

        share_w[0] = weight_of([(z, range(NY))])
        share_w[1] = weight_of([(shifted(d), range(NY)) for d in range(1, 4)] + [(shifted(4), (odd, odd + 2))])
        share_w[2] = weight_of([(shifted(-d), range(NY)) for d in range(1, 4)] + [(shifted(4), (1 - odd, 3 - odd))])

    own_slots, far_slots = NX * NY, NX * 14

    def moments(j, w_ref, low, count):
        def first(s, acc):
            return acc[0] + w_ref[low + s] * buf[j, low + s, 0], acc[1] + w_ref[low + s]

        total, weight_sum = lax.fori_loop(0, count, first, (zero, zero), unroll=True if count == 8 else 14 if count == 28 else 16)
        mean = pair_sum(total, even) / pair_sum(weight_sum, even)

        def second(s, acc):
            dev = buf[j, low + s, 0] - mean
            return acc + w_ref[low + s] * (buf[j, low + s, 1] + dev * dev)

        return mean, pair_sum(lax.fori_loop(0, count, second, zero, unroll=True if count == 8 else 14 if count == 28 else 16), even)

    def accumulate(j, w_ref, low, count, unroll, centre, spread, store):
        def prepare(s, carry):
            var_s = buf[j, low + s, 1]
            coef[0, s] = (-0.5 * LOG2E) / var_s
            coef[1, s] = w_ref[low + s] * lax.rsqrt((2.0 * math.pi) * var_s)
            return carry

        lax.fori_loop(0, count, prepare, 0, unroll=True if count == 8 else 7 if count == 28 else 16)

        for base in range(0, dens.shape[0], GROUP):
            points = [centre + offset[base + g] * spread for g in range(GROUP)]

            def add_source(s, accs):
                mean, rate, scale = buf[j, low + s, 0], coef[0, s], coef[1, s]
                out = []
                for g in range(GROUP):
                    gap = points[g] - mean
                    out.append(accs[g] + scale * jnp.exp2(gap * rate * gap))
                return tuple(out)

            accs = lax.fori_loop(0, count, add_source, (zero,) * GROUP, unroll=unroll)
            for g in range(GROUP):
                store(base + g, pair_sum(accs[g], even))

    def unpaired(x):
        return jnp.where(even, x, pltpu.roll(x, 1, 0)), jnp.where(even, pltpu.roll(x, 7, 0), x)

    tiles = 4
    width = tiles * LANES

    def put_rows(ref, row, column, value):
        for t in range(tiles):
            ref[row : row + 1, pl.ds(pl.multiple_of(column + t * LANES, LANES), LANES)] = value[2 * t : 2 * t + 1, :]

    def neighbour(side):
        return (lax.rem(z + NZ - 1 + 2 * side, NZ) * NX * NY + xl * NY + y, l)

    def received(ref, sem):
        pltpu.make_async_copy(ref, ref, sem).wait()

    def wait_blocks(j):
        count = n_cfg - NX * (3 if j < MERGED else 1)
        received(buf.at[j, pl.ds(0, count)], sem2.at[1, j])

    def send_stats(j):
        def side_stats(side, carry):
            mean, second = moments(j, wslot, own_slots + side * far_slots, far_slots)
            stat_out[j, side] = jnp.where(even, mean, second)
            return carry

        lax.fori_loop(0, 2, side_stats, 0)
        mean, second = moments(j, wslot, 0, own_slots)
        stat_own[j, 0] = mean
        stat_own[j, 1] = second
        for side in range(2):
            remote(stat_out.at[j, side], stat_in.at[j, side], sem3.at[0, j], sem3.at[1, j], neighbour(side)).start()

    def merge_stats(j):
        received(stat_in.at[j], sem3.at[1, j])
        pairs = [unpaired(stat_in[j, side]) for side in range(2)]
        means = [stat_own[j, 0]] + [p[0] for p in pairs]
        seconds = [stat_own[j, 1]] + [p[1] for p in pairs]
        shares = [share_w[i] for i in range(3)]
        centre = shares[0] * means[0] + shares[1] * means[1] + shares[2] * means[2]
        second = seconds[0] + seconds[1] + seconds[2]
        for share, mean in zip(shares, means):
            second = second + share * (mean - centre) * (mean - centre)
        spread = jnp.sqrt(second)
        line_out[j] = jnp.where(even, centre, spread)
        line_own[j, 0] = centre
        line_own[j, 1] = spread
        put_rows(mom, 0, j * width, centre)
        put_rows(mom, 1, j * width, spread)
        for side in range(2):
            remote(line_out.at[j], line_in.at[j, 1 - side], sem3.at[2, j], sem3.at[3, j], neighbour(side)).start()

    def send_parts(j):
        received(line_in.at[j], sem3.at[3, j])

        def side_part(side, carry):
            def store(row, value):
                put_rows(part_out.at[j, side], row, 0, value)

            accumulate(j, wslot, own_slots + side * far_slots, far_slots, 7, *unpaired(line_in[j, side]), store)
            return carry

        def send(side):
            remote(part_out.at[j, side], part_in.at[j, side], sem3.at[4, j], sem3.at[5, j], neighbour(side)).start()

        def store(row, value):
            put_rows(dens, row, j * width, value)

        lax.fori_loop(0, 1, side_part, 0)
        if j < 2:
            lax.fori_loop(1, 2, side_part, 0)
        accumulate(j, wslot, 0, own_slots, 8, line_own[j, 0], line_own[j, 1], store)
        send(0)
        if j >= 2:
            lax.fori_loop(1, 2, side_part, 0)
            add_parts(j - 2)
        send(1)

    def add_parts(j):
        received(part_in.at[j], sem3.at[5, j])
        lanes = pl.ds(j * width, width)
        dens[:, lanes] = mom[1:2, lanes] * (dens[:, lanes] + part_in[j, 0] + part_in[j, 1])

    def evaluate(j):
        centre, second = moments(j, wnorm, 0, n_cfg)
        spread = jnp.sqrt(second)
        put_rows(mom, 0, j * width, centre)
        put_rows(mom, 1, j * width, spread)

        def store(row, value):
            put_rows(dens, row, j * width, spread * value)

        accumulate(j, wnorm, 0, n_cfg, 8, centre, spread, store)

    def ahead(j):
        return [j + AHEAD] if j + AHEAD < CHUNKS else []

    second_hop(0, range(1, AHEAD + 1))
    send_weights()
    second_hop(1, ahead(1))
    normalize_weights()
    for step in range(1, CHUNKS + 1):
        wait_blocks(step - 1)
        if step - 1 < MERGED:
            send_stats(step - 1)
        if 0 <= step - 2 < MERGED:
            merge_stats(step - 2)
        if step + 1 < CHUNKS:
            second_hop(step + 1, ahead(step + 1))
        if 0 <= step - 3 < MERGED:
            send_parts(step - 3)
        if step - 1 >= MERGED:
            evaluate(step - 1)
        if step == CHUNKS:
            add_parts(step - 5)
    for j in range(CHUNKS - 4, MERGED):
        add_parts(j)

    def finish_first(i, carry):
        for j in range(CHUNKS):
            for a in range(2):
                pltpu.make_async_copy(relay.at[j, 0, :, :, 0, a], relay.at[j, 0, :, :, 0, a], sem1.at[j]).wait()
        return carry

    lax.fori_loop(1, n_row, finish_first, 0)
    for j in range(CHUNKS):
        count = n_cfg - NX * (3 if j < MERGED else 1)
        received(buf.at[j, pl.ds(0, count)], sem2.at[0, j])
    for j in range(MERGED):
        received(stat_out.at[j], sem3.at[0, j])
        received(line_in.at[j], sem3.at[2, j])
        received(part_out.at[j], sem3.at[4, j])

    pltpu.make_async_copy(wbuf.at[pl.ds(0, n_cfg - NX)], wbuf.at[pl.ds(0, n_cfg - NX)], wsem.at[2]).wait()


def per_device(latent_mode, latent_var, config_weight, grid_offset):
    n_cfg = lax.axis_size("cfg")
    n_lat = lax.axis_size("lat")
    own, width = latent_mode.shape
    grid = grid_offset.shape[0]
    lat_dev = width // n_cfg
    block = own * lat_dev // LANES
    size = block // CHUNKS

    def rows(a):
        a = a.reshape(own, width // LANES, LANES).transpose(1, 0, 2)
        return a.reshape(n_cfg // n_lat // (NX * NY), NX, NY, n_lat, block, LANES)

    vmem = pl.BlockSpec(memory_space=pltpu.VMEM)
    in_hbm = functools.partial(pltpu.with_memory_space_constraint, memory_space=pltpu.HBM)
    hbm = pl.BlockSpec(memory_space=pltpu.HBM)
    return pl.pallas_call(
        functools.partial(kernel, n_lat),
        out_shape=(
            jax.ShapeDtypeStruct((grid, lat_dev), jnp.float32),
            jax.ShapeDtypeStruct((2, lat_dev), jnp.float32),
        ),
        in_specs=[hbm, hbm, hbm, hbm],
        out_specs=(vmem, vmem),
        scratch_shapes=[
            pltpu.SMEM((own,), jnp.float32),
            pltpu.SMEM((grid,), jnp.float32),
            pltpu.SemaphoreType.DMA((2,)),
            pltpu.VMEM((CHUNKS, n_lat, NZ // n_lat, NY, NX, 2, size, LANES), jnp.float32),
            pltpu.VMEM((CHUNKS, n_cfg, 2, size, LANES), jnp.float32),
            pltpu.VMEM((NX, own, LANES), jnp.float32),
            pltpu.VMEM((n_cfg, own, LANES), jnp.float32),
            pltpu.VMEM((n_cfg, 8, LANES), jnp.float32),
            pltpu.VMEM((n_cfg, 8, LANES), jnp.float32),
            pltpu.VMEM((2, n_cfg, 8, LANES), jnp.float32),
            pltpu.VMEM((3, 8, LANES), jnp.float32),
            pltpu.VMEM((MERGED, 2, 8, LANES), jnp.float32),
            pltpu.VMEM((MERGED, 2, 8, LANES), jnp.float32),
            pltpu.VMEM((MERGED, 2, 8, LANES), jnp.float32),
            pltpu.VMEM((MERGED, 2, 8, LANES), jnp.float32),
            pltpu.VMEM((MERGED, 8, LANES), jnp.float32),
            pltpu.VMEM((MERGED, 2, 8, LANES), jnp.float32),
            pltpu.VMEM((MERGED, 2, grid, lat_dev // CHUNKS), jnp.float32),
            pltpu.VMEM((MERGED, 2, grid, lat_dev // CHUNKS), jnp.float32),
            pltpu.SemaphoreType.DMA((CHUNKS,)),
            pltpu.SemaphoreType.DMA((CHUNKS, n_lat)),
            pltpu.SemaphoreType.DMA((2, CHUNKS)),
            pltpu.SemaphoreType.DMA((4,)),
            pltpu.SemaphoreType.DMA((6, MERGED)),
        ],
        compiler_params=pltpu.CompilerParams(collective_id=0, has_side_effects=True, vmem_limit_bytes=52 * 1024 * 1024),
        name="mixture",
    )(rows(latent_mode), rows(latent_var), in_hbm(config_weight), in_hbm(grid_offset))


def solution(mesh):
    return jax.shard_map(
        per_device,
        mesh=mesh,
        in_specs=(P("cfg", "lat"), P("cfg", "lat"), P("cfg"), P()),
        out_specs=(P(None, ("cfg", "lat")), P(None, ("cfg", "lat"))),
        check_vma=False,
    )
```
